256 devices in a mesh: dp: 4 (over x), vocab: 64 (over z, y, core).
Axes of the slice: x: 4, y: 4, z: 8, core: 2. Of those that a mesh axis runs over, the one named last changes fastest.
Arguments:
- prefill_hidden: bfloat16 [1024, 7168], P(('dp', 'vocab')), may hold values from -60 to 60
- decode_hidden: bfloat16 [256, 7168], P(('dp', 'vocab')), may hold values from -60 to 60
- lm_head: bfloat16 [7168, 129280], P('dp', 'vocab'), as said below
- prefill_targets: int32 [1024], P(('dp', 'vocab')), may hold values from 0 to 129279
- decode_targets: int32 [256], P(('dp', 'vocab')), may hold values from 0 to 129279
- decode_live: int32 [4], P('dp'), may hold values from 1 to 64
Outputs:
- prefill_logprob: float32 [1024], P(('dp', 'vocab'))
- decode_logprob: float32 [256], P(('dp', 'vocab'))
The draws below stay inside these ranges and needn't reach their ends.
Inputs may be any that keep to these rules, and one draw needn't show every extreme that they name: `lm_head`: entries of order one over the square root of 7168.
All inputs are finite; a program needn't handle non-finite values.
Results may differ from the reference program's by a relative error of at most 0.0003.
Values may be sent and summed in bfloat16 or wider, within the bound.
A program may use at most 128 MiB of HBM per device.

```python
import jax
import jax.numpy as jnp
from jax import lax

D = 7168
VOC_DEV = 2020
VOCAB = 129280
PRE_ROWS = 1024
DEC_ROWS = 256
DEC_GROUP = 64
N_DP = 4
N_VOCAB = 64


def head_matrix(key):
    base_key = jax.random.fold_in(key, 7001)
    values = jnp.clip(jax.random.normal(jax.random.fold_in(base_key, 1), (D, VOCAB), jnp.float32), -4.0, 4.0) / jnp.sqrt(jnp.float32(D))
    return values


def draw_lm_head(key, part):
    return head_matrix(key).astype(jnp.bfloat16)


def hidden_rows(key, salt_value, row_count):
    row_key = jax.random.fold_in(key, salt_value)
    values = jnp.clip(3.0 * jax.random.normal(jax.random.fold_in(row_key, 6), (row_count, D), jnp.float32), -18.0, 18.0)
    return values.astype(jnp.bfloat16)


def draw_prefill_hidden(key, part):
    return hidden_rows(key, 11, PRE_ROWS)


def draw_decode_hidden(key, part):
    return hidden_rows(key, 13, DEC_ROWS)


def set_ends(drawn, rng, smallest, largest):
    shape = drawn.shape
    spot = [jax.random.randint(jax.random.fold_in(rng, axis), (), 0, shape[axis]) for axis in range(len(shape))]
    drawn = drawn.at[tuple(spot)].set(smallest)
    longest = shape.index(max(shape))
    spot[longest] = (spot[longest] + 1) % shape[longest]
    return drawn.at[tuple(spot)].set(largest)


def setup_inputs(seed: int = 0) -> dict:
    arg_keys = jax.random.split(jax.random.key(seed), 7)
    prefill_hidden = draw_prefill_hidden(jax.random.fold_in(arg_keys[6], 71), 0)
    decode_hidden = draw_decode_hidden(jax.random.fold_in(arg_keys[6], 71), 0)
    lm_head = draw_lm_head(jax.random.fold_in(arg_keys[6], 71), 0)
    prefill_targets = set_ends(jax.random.randint(arg_keys[3], (PRE_ROWS,), 0, VOCAB), jax.random.fold_in(arg_keys[3], 1), 0, VOCAB - 1).astype(jnp.int32)
    decode_targets = set_ends(jax.random.randint(arg_keys[4], (DEC_ROWS,), 0, VOCAB), jax.random.fold_in(arg_keys[4], 1), 0, VOCAB - 1).astype(jnp.int32)
    decode_live = set_ends(jax.random.randint(arg_keys[5], (N_DP,), 1, DEC_GROUP + 1), jax.random.fold_in(arg_keys[5], 1), 1, DEC_GROUP).astype(jnp.int32)
    return {"prefill_hidden": prefill_hidden, "decode_hidden": decode_hidden, "lm_head": lm_head, "prefill_targets": prefill_targets, "decode_targets": decode_targets, "decode_live": decode_live}


def row_logprob(hidden, targets, lm_head):
    row_count = hidden.shape[0]
    columns = jnp.arange(VOC_DEV, dtype=jnp.int32)

    def advance(running, block_index):
        row_top, totals, picked = running
        offset = (block_index * VOC_DEV).astype(jnp.int32)
        head_block = lax.dynamic_slice_in_dim(lm_head, offset, VOC_DEV, 1)
        logits = jnp.dot(hidden, head_block, preferred_element_type=jnp.float32)
        new_top = jnp.maximum(row_top, jnp.max(logits, axis=1))
        totals = totals * jnp.exp(row_top - new_top) + jnp.sum(jnp.exp(logits - new_top[:, None]), axis=1)
        target_hit = (targets - offset)[:, None] == columns[None, :]
        picked = picked + jnp.sum(jnp.where(target_hit, logits, jnp.float32(0.0)), axis=1)
        return (new_top, totals, picked), None

    initial = (jnp.full((row_count,), -jnp.inf, jnp.float32), jnp.zeros((row_count,), jnp.float32), jnp.zeros((row_count,), jnp.float32))
    (row_top, totals, picked), _ = lax.scan(advance, initial, jnp.arange(N_VOCAB, dtype=jnp.int32))
    return picked - (row_top + jnp.log(totals))


def reference(prefill_hidden, decode_hidden, lm_head, prefill_targets, decode_targets, decode_live):
    prefill_logprob = row_logprob(prefill_hidden, prefill_targets, lm_head)
    decode_values = row_logprob(decode_hidden, decode_targets, lm_head)
    positions = jnp.arange(DEC_ROWS, dtype=jnp.int32)
    group_live = decode_live[positions // DEC_GROUP]
    decode_logprob = jnp.where(positions % DEC_GROUP < group_live, decode_values, jnp.float32(0.0))
    return prefill_logprob, decode_logprob
```

```python
import jax
import jax.numpy as jnp
from jax import lax
from jax.experimental import pallas as pl
from jax.experimental.pallas import tpu as pltpu
from jax.sharding import Mesh
from jax.sharding import PartitionSpec as P

VOCAB = ("z", "y", "c")
DP_VOCAB = ("dp", "z", "y", "c")
MESH = pl.DeviceIdType.MESH
GROUP = 16
TOP = 32000.0
STAT = 256


def make_kernel(nx, nz, ny, nc, rows, depth, vocab):
    pieces_n = nx * nc
    small = pieces_n * rows
    block = ny * small
    half = block // 2
    padded = -(-vocab // 512) * 512
    last = padded - 128
    nb = nz // nx

    def kernel(pre_ref, dec_ref, pt_ref, dt_ref, w_hbm, out_ref,
               w, pieces, xrecv, f40, ybuf, fblk, hall, part, sbuf, relay, rdst,
               stat, tt, st, cst, yst, zst, res,
               w_sem, xs, xr, ys, yr, ags, agr, d2s, d2r, ts, tr, rs, rlr, rdr,
               cs, cr, y2s, y2r, z2s, z2r, x2s, x2r):
        x = lax.axis_index("dp")
        z = lax.axis_index("z")
        y = lax.axis_index("y")
        c = lax.axis_index("c")
        other = 1 - c
        me = x * nc + c
        w_copy = pltpu.make_async_copy(w_hbm, w, w_sem)
        w_copy.start()

        def send(src, dst, ssem, rsem, dev):
            return pltpu.make_async_remote_copy(
                src_ref=src, dst_ref=dst, send_sem=ssem, recv_sem=rsem,
                device_id=dev, device_id_type=MESH)

        def arrival(dst, sem):
            return send(dst, dst, sem, sem, (x, z, y, other))

        barrier = pltpu.get_barrier_semaphore()
        peers = []
        for k in range(1, pieces_n):
            p = lax.rem(me + k, pieces_n)
            peers.append((lax.div(p, nc), z, y, lax.rem(p, nc)))
        for k in range(1, ny):
            peers.append((x, z, lax.rem(y + k, ny), c))
        for k in range(1, nz):
            peers.append((x, lax.rem(z + k, nz), y, c))
        for dev in peers:
            pl.semaphore_signal(barrier, inc=1, device_id=dev, device_id_type=MESH)

        n_pre = pre_ref.shape[0]
        n_dec = dec_ref.shape[0]
        for p in range(pieces_n):
            cols = slice(p * depth, (p + 1) * depth)
            pieces[p, 0:n_pre, 0:depth] = pre_ref[:, cols].astype(jnp.float32)
            pieces[p, n_pre:rows, 0:depth] = dec_ref[:, cols].astype(jnp.float32)
        for r in range(rows):
            t = pt_ref[r] if r < n_pre else dt_ref[r - n_pre]
            tv = jnp.full((1, 128), t, jnp.int32).astype(jnp.float32)
            for p in range(pieces_n):
                pieces[p, r:r + 1, depth:depth + 128] = tv
        for p in range(pieces_n):
            pieces[p, rows:8, :] = jnp.zeros((8 - rows, depth + 128), jnp.float32)
        for k in range(nz):
            for h in range(2):
                part[k, h, :, last:padded] = jnp.zeros((half, 128), jnp.float32)
        stat[...] = jnp.zeros(stat.shape, jnp.float32)

        pl.semaphore_wait(barrier, len(peers))

        def x_copy(k):
            p = lax.rem(me + k, pieces_n)
            return send(pieces.at[p], xrecv.at[me], xs.at[p], xr.at[me],
                        (lax.div(p, nc), z, y, lax.rem(p, nc)))

        for k in range(1, pieces_n):
            x_copy(k).start()
        xrecv[me] = pieces[me]
        for k in range(1, pieces_n):
            p = lax.rem(me + k, pieces_n)
            arrival(xrecv.at[p], xr.at[p]).wait_recv()
        for s in range(pieces_n):
            f40[s * rows:(s + 1) * rows, :] = xrecv[s, 0:rows, :]

        lane = lax.broadcasted_iota(jnp.int32, (small, 128), 1)
        tcol = f40[:, depth:depth + 128]
        t1 = jnp.floor(tcol * (1.0 / 256.0))
        t2 = jnp.floor(t1 * (1.0 / 256.0))
        digits = jnp.where(lane == 0, tcol - 256.0 * t1,
                           jnp.where(lane == 1, t1 - 256.0 * t2,
                                     jnp.where(lane == 2, t2, 0.0)))
        ybuf[y, :, 0:depth] = f40[:, 0:depth].astype(jnp.bfloat16)
        ybuf[y, :, depth:depth + 128] = digits.astype(jnp.bfloat16)

        def y_copy(k):
            yy = lax.rem(y + k, ny)
            return send(ybuf.at[y], ybuf.at[y], ys.at[yy], yr.at[y], (x, z, yy, c))

        for k in range(1, ny):
            y_copy(k).start()
        for k in range(1, ny):
            yy = lax.rem(y + k, ny)
            arrival(ybuf.at[yy], yr.at[yy]).wait_recv()
        for s in range(ny):
            fblk[s * small:(s + 1) * small, :] = ybuf[s].astype(jnp.float32)
        hall[c, z] = fblk[:, 0:depth].astype(jnp.bfloat16)

        def own_copy(way):
            zz = lax.rem(z + (1 if way else nz - 1), nz)
            return send(hall.at[c, z], hall.at[c, z], ags.at[nz if way else z], agr.at[z],
                        (x, zz, y, c))

        def core_copy(zb):
            return send(hall.at[c, zb], hall.at[c, zb], d2s.at[zb], d2r.at[zb], (x, z, y, other))

        own_copy(0).start()
        own_copy(1).start()
        core_copy(z).start()

        slot = lax.div(z, nx)
        reducer = lax.rem(z, nx) == x
        digit = lax.broadcasted_iota(jnp.int32, (block, 128), 1)
        weight = jnp.where(digit == 0, 1.0, jnp.where(digit == 1, 256.0,
                                                      jnp.where(digit == 2, 65536.0, 0.0)))
        ids = jnp.sum(fblk[:, depth:depth + 128] * weight, axis=1, keepdims=True)
        stat[0:block, :] = jnp.broadcast_to(ids, (block, 128))

        def tile_of():
            for k in range(STAT // 128):
                yield k, jnp.transpose(stat[k * 128:(k + 1) * 128, :])[0:8, :]

        def t_copy(k):
            zz = lax.rem(z + k, nz)
            return send(tt.at[slot], tt.at[slot], ts.at[zz], tr.at[slot], (x, zz, y, c))

        @pl.when(reducer)
        def _():
            for k, tile in tile_of():
                tt[slot, :, k * 128:(k + 1) * 128] = tile
            for k in range(1, nz):
                t_copy(k).start()

        w_copy.wait()

        def offset(i):
            odd = lax.rem(i, 2)
            dist = lax.div(i + 1, 2)
            zb = lax.rem(z + nz + jnp.where(odd == 1, dist, -dist), nz)
            return odd, dist, zb

        def role_of(zb):
            return lax.rem(x + nx * nz - zb, nx)

        def forward(i):
            odd, dist, zb = offset(i)
            zz = lax.rem(z + jnp.where(odd == 1, nz - 1, 1), nz)
            go = dist < jnp.where(odd == 1, nz // 2, nz - nz // 2 - 1)
            copy = send(hall.at[c, zb], hall.at[c, zb], ags.at[zb], agr.at[zb], (x, zz, y, c))
            return jnp.logical_and(i > 0, go), copy

        def quantise(zb, h, relayed):
            @pl.loop(0, half // GROUP)
            def _(g):
                at = pl.ds(pl.multiple_of(g * GROUP, GROUP), GROUP)
                v = part[zb, h, at, :]
                if relayed:
                    v = v + unpack(relay[zb, at, :])
                big = jnp.max(jnp.abs(v), axis=1, keepdims=True)
                e = jnp.ceil(jnp.log2(jnp.maximum(big, 1e-20) * (1.0 / TOP)))
                q = jnp.round(v * jnp.exp2(-e))
                tail = lax.broadcasted_iota(jnp.int32, q.shape, 1) >= vocab
                q = jnp.where(tail, e, q)
                sbuf[zb, h, at, :] = q.astype(jnp.int32).astype(jnp.int16)

        def unpack(code):
            v = code.astype(jnp.int32).astype(jnp.float32)
            e = v[:, padded - 1:padded]
            tail = lax.broadcasted_iota(jnp.int32, v.shape, 1) >= vocab
            return jnp.where(tail, 0.0, v * jnp.exp2(e))

        def relay_copy(zb, h):
            xx = lax.rem(x + jnp.where(h == 0, nx - 1, 1), nx)
            return send(sbuf.at[zb, h], relay.at[zb], rs.at[zb, h], rlr.at[zb], (xx, z, y, c))

        def final_copy(zb, h, side):
            xx = lax.rem(x + jnp.where(side == 0, nx - 1, 1), nx)
            b = lax.div(zb, nx)
            return send(sbuf.at[zb, h], rdst.at[b, side, h], rs.at[zb, h], rdr.at[b, side, h],
                        (xx, z, y, c))

        def step(i, carry):
            odd, dist, zb = offset(i)

            @pl.when(i > 0)
            def _():
                arrival(hall.at[c, zb], agr.at[zb]).wait_recv()
                core_copy(zb).start()

            go, copy = forward(i)

            @pl.when(go)
            def _():
                copy.start()

            arrival(hall.at[other, zb], d2r.at[zb]).wait_recv()
            for n in range(padded // 512):
                n0, n1 = n * 512, min(n * 512 + 512, vocab)
                acc = jnp.dot(hall[0, zb], w[0:depth, n0:n1], preferred_element_type=jnp.float32)
                acc += jnp.dot(hall[1, zb], w[depth:2 * depth, n0:n1],
                               preferred_element_type=jnp.float32)
                part[zb, 0, :, n0:n1] = acc[0:half]
                part[zb, 1, :, n0:n1] = acc[half:block]
            role = role_of(zb)

            @pl.when(role == 2)
            def _():
                for h in range(2):
                    quantise(zb, h, False)
                    relay_copy(zb, h).start()

            @pl.when(lax.rem(role, 2) == 1)
            def _():
                h = jnp.where(role == 1, 1, 0)
                quantise(zb, h, False)
                final_copy(zb, h, jnp.where(role == 1, 0, 1)).start()

            return carry

        lax.fori_loop(0, nz, step, 0)

        def pass_on(i, carry):
            odd, dist, zb = offset(i)
            role = role_of(zb)

            @pl.when(lax.rem(role, 2) == 1)
            def _():
                h = jnp.where(role == 1, 0, 1)
                arrival(relay.at[zb], rlr.at[zb]).wait_recv()
                quantise(zb, h, True)
                final_copy(zb, h, jnp.where(role == 1, 0, 1)).start()

            return carry

        lax.fori_loop(0, nz, pass_on, 0)

        first = ((z * ny + y) * nc + c) * vocab
        firstf = first.astype(jnp.float32)

        def reduce(b, carry):
            zb = x + nx * b

            @pl.when(zb != z)
            def _():
                arrival(tt.at[b], tr.at[b]).wait_recv()

            for k in range(STAT // 128):
                cols = jnp.broadcast_to(tt[b, 0:1, k * 128:(k + 1) * 128], (128, 128))
                stat[k * 128:(k + 1) * 128, :] = jnp.transpose(cols)
            for h in range(2):
                for side in range(2):
                    arrival(rdst.at[b, side, h], rdr.at[b, side, h]).wait_recv()

                @pl.loop(0, half // GROUP)
                def _(g):
                    at = pl.ds(pl.multiple_of(g * GROUP, GROUP), GROUP)
                    rat = pl.ds(pl.multiple_of(h * half + g * GROUP, GROUP), GROUP)
                    v = part[zb, h, at, :] + (unpack(rdst[b, 0, h, at, :])
                                              + unpack(rdst[b, 1, h, at, :]))
                    col = lax.broadcasted_iota(jnp.int32, v.shape, 1)
                    local = (stat[rat, 0:1] - firstf).astype(jnp.int32)
                    picked = jnp.sum(jnp.where(col == local, v, 0.0), axis=1, keepdims=True)
                    v = jnp.where(col >= vocab, -jnp.inf, v)
                    top = jnp.max(v, axis=1, keepdims=True)
                    total = jnp.sum(jnp.exp(v - top), axis=1, keepdims=True)
                    ln = lax.broadcasted_iota(jnp.int32, (GROUP, 128), 1)
                    picked = jnp.where(jnp.logical_and(local >= 0, local < vocab), picked, 0.0)
                    stat[rat, :] = jnp.where(ln == 0, top, jnp.where(ln == 1, total,
                                                                    jnp.where(ln == 2, picked, 0.0)))
            for k, tile in tile_of():
                st[b, :, k * 128:(k + 1) * 128] = tile
            return carry

        lax.fori_loop(0, nb, reduce, 0)

        def join(tiles):
            tops = [t[0:1, :] for t in tiles]
            top = tops[0]
            for t in tops[1:]:
                top = jnp.maximum(top, t)
            total, picked = 0.0, 0.0
            for t, m in zip(tiles, tops):
                total += t[1:2, :] * jnp.exp(m - top)
                picked += t[2:3, :]
            return top, total, picked

        def put(ref, joined):
            top, total, picked = joined
            row = lax.broadcasted_iota(jnp.int32, (8, STAT), 0)
            ref[...] = jnp.where(row == 0, top, jnp.where(row == 1, total,
                                                          jnp.where(row == 2, picked, 0.0)))

        c_copy = send(st.at[other], cst, cs, cr, (x, z, y, other))
        c_copy.start()
        arrival(cst, cr).wait_recv()
        put(yst.at[y], join([st[c], cst[...]]))

        def y2_copy(k):
            yy = lax.rem(y + k, ny)
            return send(yst.at[y], yst.at[y], y2s.at[yy], y2r.at[y], (x, z, yy, c))

        for k in range(1, ny):
            y2_copy(k).start()
        for k in range(1, ny):
            yy = lax.rem(y + k, ny)
            arrival(yst.at[yy], y2r.at[yy]).wait_recv()
        put(zst.at[z], join([yst[k] for k in range(ny)]))
        home = x + nx * c
        z2_copy = send(zst.at[z], zst.at[z], z2s, z2r.at[z], (x, home, y, c))

        @pl.when(z != home)
        def _():
            z2_copy.start()

        def x2_copy(k):
            p = lax.rem(me + k, pieces_n)
            return send(res, out_ref, x2s.at[p], x2r, (lax.div(p, nc), z, y, lax.rem(p, nc)))

        @pl.when(z == home)
        def _():
            for k in range(1, nz):
                zz = lax.rem(z + k, nz)
                arrival(zst.at[zz], z2r.at[zz]).wait_recv()
            top, total, picked = join([zst[k] for k in range(nz)])
            value = jnp.broadcast_to(picked - (top + jnp.log(total)), (8, STAT))
            res[...] = value
            for k in range(1, pieces_n):
                x2_copy(k).start()
            out_ref[...] = value

        @pl.when(z != home)
        def _():
            arrival(out_ref, x2r).wait_recv()

        for k in range(1, pieces_n):
            x_copy(k).wait_send()
        for k in range(1, ny):
            y_copy(k).wait_send()
            y2_copy(k).wait_send()
        own_copy(0).wait_send()
        own_copy(1).wait_send()
        c_copy.wait_send()

        @pl.when(reducer)
        def _():
            for k in range(1, nz):
                t_copy(k).wait_send()

        def drain(i, carry):
            odd, dist, zb = offset(i)
            core_copy(zb).wait_send()
            go, copy = forward(i)

            @pl.when(go)
            def _():
                copy.wait_send()

            @pl.when(role_of(zb) != 0)
            def _():
                for h in range(2):
                    relay_copy(zb, h).wait_send()

            return carry

        lax.fori_loop(0, nz, drain, 0)

        @pl.when(z != home)
        def _():
            z2_copy.wait_send()

        @pl.when(z == home)
        def _():
            for k in range(1, pieces_n):
                x2_copy(k).wait_send()

    f32, bf16, i16 = jnp.float32, jnp.bfloat16, jnp.int16
    dma = pltpu.SemaphoreType.DMA
    scratch = [
        pltpu.VMEM((2 * depth, vocab), bf16),
        pltpu.VMEM((pieces_n, 8, depth + 128), f32),
        pltpu.VMEM((pieces_n, 8, depth + 128), f32),
        pltpu.VMEM((small, depth + 128), f32),
        pltpu.VMEM((ny, small, depth + 128), bf16),
        pltpu.VMEM((block, depth + 128), f32),
        pltpu.VMEM((nc, nz, block, depth), bf16),
        pltpu.VMEM((nz, 2, half, padded), f32),
        pltpu.VMEM((nz, 2, half, padded), i16),
        pltpu.VMEM((nz, half, padded), i16),
        pltpu.VMEM((nb, 2, 2, half, padded), i16),
        pltpu.VMEM((STAT, 128), f32),
        pltpu.VMEM((nb, 8, STAT), f32),
        pltpu.VMEM((nb, 8, STAT), f32),
        pltpu.VMEM((8, STAT), f32),
        pltpu.VMEM((ny, 8, STAT), f32),
        pltpu.VMEM((nz, 8, STAT), f32),
        pltpu.VMEM((8, STAT), f32),
        dma, dma((pieces_n,)), dma((pieces_n,)), dma((ny,)), dma((ny,)),
        dma((nz + 1,)), dma((nz,)), dma((nz,)), dma((nz,)), dma((nz,)), dma((nb,)),
        dma((nz, 2)), dma((nz,)), dma((nb, 2, 2)),
        dma, dma, dma((ny,)), dma((ny,)), dma, dma((nz,)), dma((pieces_n,)), dma,
    ]
    return kernel, scratch


def body(prefill_hidden, decode_hidden, lm_head, prefill_targets, decode_targets, decode_live):
    nx, nz = lax.axis_size("dp"), lax.axis_size("z")
    ny, nc = lax.axis_size("y"), lax.axis_size("c")
    pre, dec = prefill_hidden.shape[0], decode_hidden.shape[0]
    rows = pre + dec
    width, vocab = lm_head.shape
    kernel, scratch = make_kernel(nx, nz, ny, nc, rows, width // nc, vocab)
    vmem = pl.BlockSpec(memory_space=pltpu.VMEM)
    smem = pl.BlockSpec(memory_space=pltpu.SMEM)
    values = pl.pallas_call(
        kernel,
        out_shape=jax.ShapeDtypeStruct((8, STAT), jnp.float32),
        in_specs=[vmem, vmem, smem, smem, pl.BlockSpec(memory_space=pl.ANY)],
        out_specs=vmem,
        scratch_shapes=scratch,
        compiler_params=pltpu.CompilerParams(
            collective_id=0, has_side_effects=True, vmem_limit_bytes=60 << 20),
    )(prefill_hidden, decode_hidden, prefill_targets, decode_targets, lm_head)
    x, y, c = lax.axis_index("dp"), lax.axis_index("y"), lax.axis_index("c")
    at = (y * (nx * nc) + x * nc + c) * rows
    own = lax.dynamic_slice_in_dim(values[0], at, rows, 0)
    positions = lax.axis_index(VOCAB) * dec + jnp.arange(dec, dtype=jnp.int32)
    decode = jnp.where(positions < decode_live[0], own[pre:], jnp.float32(0.0))
    return own[:pre], decode


def solution(mesh):
    split = Mesh(mesh.devices.reshape(mesh.shape["dp"], 8, 4, 2), DP_VOCAB)
    placed = (
        P(DP_VOCAB, None),
        P(DP_VOCAB, None),
        P("dp", VOCAB),
        P(DP_VOCAB),
        P(DP_VOCAB),
        P("dp"),
    )
    return jax.shard_map(
        body, mesh=split, in_specs=placed, out_specs=(P(DP_VOCAB), P(DP_VOCAB)), check_vma=False
    )
```

```python
import jax
import jax.numpy as jnp
from jax import lax
from jax.experimental import pallas as pl
from jax.experimental.pallas import tpu as pltpu
from jax.sharding import Mesh
from jax.sharding import PartitionSpec as P

VOCAB = ("z", "y", "c")
DP_VOCAB = ("dp", "z", "y", "c")
MESH = pl.DeviceIdType.MESH
LANES = 128
CHUNK = 256
TOP = 32000.0


def make_kernel(nx, nz, ny, nc, rows, depth, vocab):
    pieces_n = nx * nc
    small = pieces_n * rows
    block = ny * small
    first_n = vocab // 32 * 16
    counts = (first_n, vocab - first_n)
    width = -(-(max(counts) + 1) // 512) * 512
    plane = nz * ny * nc

    def kernel(pre_ref, dec_ref, pt_ref, dt_ref, w_hbm, out_ref,
               w, pieces, xrecv, f40, ybuf, fblk, hall, part, sbuf, rel, rd,
               stat, tt, st, fin, res,
               w_sem, xs, xr, ys, yr, yf, yfr, ags, agr, d2s, d2r, ts, tr, rs, rlr, rdr,
               fs, fr, x2s, x2r):
        x = lax.axis_index("dp")
        z = lax.axis_index("z")
        y = lax.axis_index("y")
        c = lax.axis_index("c")
        other = 1 - c
        me = x * nc + c
        right = (lax.rem(x + 1, nx), z, y, c)
        left = (lax.rem(x + nx - 1, nx), z, y, c)
        w_copy = pltpu.make_async_copy(w_hbm, w, w_sem)
        w_copy.start()

        def send(src, dst, ssem, rsem, dev):
            return pltpu.make_async_remote_copy(
                src_ref=src, dst_ref=dst, send_sem=ssem, recv_sem=rsem,
                device_id=dev, device_id_type=MESH)

        def arrival(dst, sem):
            return send(dst, dst, sem, sem, (x, z, y, other))

        barrier = pltpu.get_barrier_semaphore()
        peers = []
        for k in range(1, pieces_n):
            p = lax.rem(me + k, pieces_n)
            peers.append((lax.div(p, nc), z, y, lax.rem(p, nc)))
        for k in range(1, ny):
            peers.append((x, z, lax.rem(y + k, ny), c))
        for k in (1, nz - 1):
            peers.append((x, lax.rem(z + k, nz), y, c))
        for dev in peers:
            pl.semaphore_signal(barrier, inc=1, device_id=dev, device_id_type=MESH)

        n_pre = pre_ref.shape[0]
        lane = lax.broadcasted_iota(jnp.int32, (rows, LANES), 1)
        row = lax.broadcasted_iota(jnp.int32, (rows, LANES), 0)
        ids = jnp.zeros((rows, LANES), jnp.int32)
        for r in range(rows):
            ids = jnp.where(row == r, pt_ref[r] if r < n_pre else dt_ref[r - n_pre], ids)
        digits = jnp.where(lane == 0, ids % 256,
                           jnp.where(lane == 1, (ids // 256) % 256,
                                     jnp.where(lane == 2, ids // 65536, 0))).astype(jnp.float32)
        for p in range(pieces_n):
            cols = slice(p * depth, (p + 1) * depth)
            own = jnp.concatenate([pre_ref[:, cols].astype(jnp.float32),
                                   dec_ref[:, cols].astype(jnp.float32)], axis=0)
            pieces[p, :, 0:depth] = own.astype(jnp.bfloat16)
            pieces[p, :, depth:depth + LANES] = digits.astype(jnp.bfloat16)
        for k in range(nz):
            for h in range(2):
                part[k, h, :, width - LANES:width] = jnp.zeros((block, LANES), jnp.float32)
        stat[...] = jnp.zeros(stat.shape, jnp.float32)

        pl.semaphore_wait(barrier, len(peers))

        def x_copy(k):
            p = lax.rem(me + k, pieces_n)
            return send(pieces.at[p], xrecv.at[me], xs.at[p], xr.at[me],
                        (lax.div(p, nc), z, y, lax.rem(p, nc)))

        for k in range(1, pieces_n):
            x_copy(k).start()
        xrecv[me] = pieces[me]
        for k in range(1, pieces_n):
            p = lax.rem(me + k, pieces_n)
            arrival(xrecv.at[p], xr.at[p]).wait_recv()
        for s in range(pieces_n):
            f40[s * rows:(s + 1) * rows, :] = xrecv[s].astype(jnp.float32)

        ybuf[y] = f40[...].astype(jnp.bfloat16)
        up, down = lax.rem(y + 1, ny), lax.rem(y + ny - 1, ny)
        mid = (depth + LANES) // 2

        def y_copy(way):
            return send(ybuf.at[y], ybuf.at[y], ys.at[way], yr.at[way],
                        (x, z, up if way else down, c))

        def y_forward(way):
            src = ybuf.at[down if way else up, :, pl.ds(way * mid, mid)]
            return send(src, src, yf.at[way], yfr.at[way], (x, z, up if way else down, c))

        y_copy(0).start()
        y_copy(1).start()
        for way in (1, 0):
            arrival(ybuf.at[down if way else up], yr.at[way]).wait_recv()
            y_forward(way).start()
        far = lax.rem(y + 2, ny)
        for way in (1, 0):
            arrival(ybuf.at[far, :, pl.ds(way * mid, mid)], yfr.at[way]).wait_recv()
        for s in range(ny):
            fblk[s * small:(s + 1) * small, :] = ybuf[s].astype(jnp.float32)
        hall[c, z] = fblk[:, 0:depth].astype(jnp.bfloat16)

        def own_copy(way):
            zz = lax.rem(z + (1 if way else nz - 1), nz)
            return send(hall.at[c, z], hall.at[c, z], ags.at[nz if way else z], agr.at[z],
                        (x, zz, y, c))

        def core_copy(zb):
            return send(hall.at[c, zb], hall.at[c, zb], d2s.at[zb], d2r.at[zb], (x, z, y, other))

        own_copy(0).start()
        own_copy(1).start()
        core_copy(z).start()

        digit = lax.broadcasted_iota(jnp.int32, (small, LANES), 1)
        weight = jnp.where(digit == 0, 1.0, jnp.where(digit == 1, 256.0,
                                                      jnp.where(digit == 2, 65536.0, 0.0)))
        at_x = pl.ds(pl.multiple_of(x * small, 8), small)
        named = jnp.sum(fblk[at_x, depth:depth + LANES] * weight, axis=1, keepdims=True)
        stat[0:small, :] = jnp.broadcast_to(named, (small, LANES))
        tt[z] = jnp.transpose(stat[...])[0:8, :]

        w_copy.wait()

        def block_of(i):
            odd = lax.rem(i, 2)
            dist = lax.div(i + 1, 2)
            return lax.rem(z + nz + jnp.where(odd == 1, dist, -dist), nz)

        def forward(dist, way):
            zb = lax.rem(z + nz + (-dist if way else dist), nz)
            zz = lax.rem(z + (1 if way else nz - 1), nz)
            return send(hall.at[c, zb], hall.at[c, zb], ags.at[zb], agr.at[zb], (x, zz, y, c))

        def product(rows_of, columns_of):
            return lax.dot_general(rows_of, columns_of, (((1,), (1,)), ((), ())),
                                   preferred_element_type=jnp.float32)

        def multiply(blocks):
            for h in range(2):
                base = h * first_n
                for n0 in range(0, counts[h], 512):
                    n1 = min(n0 + 512, counts[h])
                    at = slice(base + n0, base + n1)
                    lhs = [jnp.concatenate([hall[k, zb] for zb in blocks], axis=0)
                           if len(blocks) > 1 else hall[k, blocks[0]] for k in range(2)]
                    acc = product(lhs[0], w[at, 0:depth]) + product(lhs[1], w[at, depth:2 * depth])
                    for j, zb in enumerate(blocks):
                        part[zb, h, :, n0:n1] = acc[j * block:(j + 1) * block]

        def rows_at(q):
            return pl.ds(pl.multiple_of(q * small, 8), small)

        def step_of(code, h):
            return jnp.exp2(code[:, LANES - 1:LANES].astype(jnp.int32).astype(jnp.float32))

        def unpack(code, n0, h, step):
            v = code.astype(jnp.int32).astype(jnp.float32) * step
            if n0 + CHUNK > counts[h]:
                col = lax.broadcasted_iota(jnp.int32, v.shape, 1)
                v = jnp.where(col >= counts[h] - n0, 0.0, v)
            return v

        def quantise(zb, h, q, slot, relayed):
            at = rows_at(q)
            big = jnp.zeros((small, LANES), jnp.float32)
            if relayed:
                step = step_of(rel[zb, h, :, width - LANES:width], h)
            for n0 in range(0, width, CHUNK):
                v = part[zb, h, at, n0:n0 + CHUNK]
                if relayed:
                    v = v + unpack(rel[zb, h, :, n0:n0 + CHUNK], n0, h, step)
                    part[zb, h, at, n0:n0 + CHUNK] = v
                for k in range(0, CHUNK, LANES):
                    big = jnp.maximum(big, jnp.abs(v[:, k:k + LANES]))
            big = jnp.max(big, axis=1, keepdims=True)
            e = jnp.ceil(jnp.log2(jnp.maximum(big, 1e-20) * (1.0 / TOP)))
            scale = jnp.exp2(-e)
            for n0 in range(0, width, CHUNK):
                v = jnp.round(part[zb, h, at, n0:n0 + CHUNK] * scale)
                if n0 + CHUNK > counts[h]:
                    col = lax.broadcasted_iota(jnp.int32, v.shape, 1)
                    v = jnp.where(col >= counts[h] - n0, e, v)
                sbuf[zb, slot, :, n0:n0 + CHUNK] = v.astype(jnp.int32).astype(jnp.int16)

        toward_left = lax.rem(x + nx - 1, nx)
        toward_right = lax.rem(x + 1, nx)
        opposite = lax.rem(x + 2, nx)

        def message(zb, slot):
            if slot == 0:
                dst, rsem, dev = rel.at[zb, 0], rlr.at[zb, 0], left
            elif slot == 1:
                dst, rsem, dev = rel.at[zb, 1], rlr.at[zb, 1], right
            elif slot in (2, 4):
                h = 1 if slot == 2 else 0
                dst, rsem, dev = rd.at[zb, 0, h], rdr.at[zb, 0, h], left
            else:
                h = 0 if slot == 3 else 1
                dst, rsem, dev = rd.at[zb, 1, h], rdr.at[zb, 1, h], right
            return send(sbuf.at[zb, slot], dst, rs.at[zb, slot], rsem, dev)

        def emit(zb):
            for slot, h, q in ((0, 0, opposite), (1, 1, opposite),
                               (2, 1, toward_left), (3, 0, toward_right)):
                quantise(zb, h, q, slot, False)
                message(zb, slot).start()

        arrival(hall.at[other, z], d2r.at[z]).wait_recv()
        multiply([z])
        emit(z)

        def pair(dist, carry):
            above = lax.rem(z + dist, nz)
            below = lax.rem(z + nz - dist, nz)
            arrival(hall.at[c, above], agr.at[above]).wait_recv()
            core_copy(above).start()
            forward(dist, 0).start()
            arrival(hall.at[c, below], agr.at[below]).wait_recv()
            core_copy(below).start()

            @pl.when(dist < nz // 2 - 1)
            def _():
                forward(dist, 1).start()

            arrival(hall.at[other, above], d2r.at[above]).wait_recv()
            arrival(hall.at[other, below], d2r.at[below]).wait_recv()
            multiply([above, below])

            def one(j, carry):
                emit(jnp.where(j == 0, above, below))
                return carry

            lax.fori_loop(0, 2, one, 0)
            return carry

        lax.fori_loop(1, nz // 2, pair, 0)
        across = lax.rem(z + nz // 2, nz)
        arrival(hall.at[c, across], agr.at[across]).wait_recv()
        core_copy(across).start()
        arrival(hall.at[other, across], d2r.at[across]).wait_recv()
        multiply([across])
        emit(across)

        def t_copy(k):
            zz = lax.rem(z + k, nz)
            return send(tt.at[z], tt.at[z], ts.at[zz], tr.at[z], (x, zz, y, c))

        for k in range(1, nz):
            t_copy(k).start()

        def pass_on(i, carry):
            zb = block_of(i)
            arrival(rel.at[zb, 0], rlr.at[zb, 0]).wait_recv()
            quantise(zb, 0, toward_left, 4, True)
            message(zb, 4).start()
            arrival(rel.at[zb, 1], rlr.at[zb, 1]).wait_recv()
            quantise(zb, 1, toward_right, 5, True)
            message(zb, 5).start()
            return carry

        lax.fori_loop(0, nz, pass_on, 0)
        for k in range(1, nz):
            zz = lax.rem(z + k, nz)
            arrival(tt.at[zz], tr.at[zz]).wait_recv()

        first = (((z * ny + y) * nc + c) * vocab).astype(jnp.float32)
        mine = (z * ny + y) * nc + c
        at_row = rows_at(x)

        def home_of(zb):
            return (x, zb, x, lax.div(zb * nc, nz))

        def f_copy(zb):
            return send(st.at[zb], fin.at[mine], fs.at[zb], fr, home_of(zb))

        def is_home(zb):
            return jnp.logical_and(jnp.logical_and(z == zb, y == x), c == lax.div(zb * nc, nz))

        def reduce(i, carry):
            zb = block_of(i)
            wanted = jnp.transpose(jnp.broadcast_to(tt[zb, 0:1, :], (LANES, LANES)))[0:small, 0:1]
            big = jnp.full((small, LANES), -jnp.inf, jnp.float32)
            picked = jnp.zeros((small, LANES), jnp.float32)
            for h in range(2):
                for side in range(2):
                    arrival(rd.at[zb, side, h], rdr.at[zb, side, h]).wait_recv()
                steps = [step_of(rd[zb, side, h, :, width - LANES:width], h) for side in range(2)]
                local = (wanted - (first + float(h * first_n))).astype(jnp.int32)
                local = jnp.where(jnp.logical_and(local >= 0, local < counts[h]), local, -1)
                for n0 in range(0, width, CHUNK):
                    at = slice(n0, n0 + CHUNK)
                    v = part[zb, h, at_row, at] + (unpack(rd[zb, 0, h, :, at], n0, h, steps[0])
                                                   + unpack(rd[zb, 1, h, :, at], n0, h, steps[1]))
                    col = lax.broadcasted_iota(jnp.int32, v.shape, 1)
                    hit = jnp.where(col == local - n0, v, 0.0)
                    if n0 + CHUNK > counts[h]:
                        v = jnp.where(col >= counts[h] - n0, -jnp.inf, v)
                    part[zb, h, at_row, at] = v
                    for k in range(0, CHUNK, LANES):
                        big = jnp.maximum(big, v[:, k:k + LANES])
                        picked = picked + hit[:, k:k + LANES]
            top = jnp.max(big, axis=1, keepdims=True)
            total = jnp.zeros((small, LANES), jnp.float32)
            for h in range(2):
                for n0 in range(0, width, CHUNK):
                    v = jnp.exp(part[zb, h, at_row, n0:n0 + CHUNK] - top)
                    for k in range(0, CHUNK, LANES):
                        total = total + v[:, k:k + LANES]
            total = jnp.sum(total, axis=1, keepdims=True)
            picked = jnp.sum(picked, axis=1, keepdims=True)
            ln = lax.broadcasted_iota(jnp.int32, (small, LANES), 1)
            stat[0:small, :] = jnp.where(ln == 0, top, jnp.where(ln == 1, total,
                                                                jnp.where(ln == 2, picked, 0.0)))
            tile = jnp.transpose(stat[...])[0:3, :]
            st[zb] = tile

            @pl.when(is_home(zb))
            def _():
                fin[mine] = tile

            @pl.when(jnp.logical_not(is_home(zb)))
            def _():
                f_copy(zb).start()

            return carry

        lax.fori_loop(0, nz, reduce, 0)

        home = is_home(z)

        def x2_copy(k):
            p = lax.rem(me + k, pieces_n)
            return send(res, out_ref, x2s.at[p], x2r, (lax.div(p, nc), z, y, lax.rem(p, nc)))

        @pl.when(home)
        def _():
            arrival(fin.at[0:plane - 1], fr).wait_recv()
            tops = fin[:, 0, :]
            top = jnp.max(tops, axis=0, keepdims=True)
            total = jnp.sum(fin[:, 1, :] * jnp.exp(tops - top), axis=0, keepdims=True)
            picked = jnp.sum(fin[:, 2, :], axis=0, keepdims=True)
            value = jnp.broadcast_to(picked - (top + jnp.log(total)), (8, LANES))
            res[...] = value
            for k in range(1, pieces_n):
                x2_copy(k).start()
            out_ref[...] = value

        @pl.when(jnp.logical_not(home))
        def _():
            arrival(out_ref, x2r).wait_recv()

        for k in range(1, pieces_n):
            x_copy(k).wait_send()
        for way in range(2):
            y_copy(way).wait_send()
            y_forward(way).wait_send()
            own_copy(way).wait_send()
        for k in range(1, nz):
            t_copy(k).wait_send()

        def drain(i, carry):
            zb = block_of(i)
            core_copy(zb).wait_send()
            for slot in range(6):
                message(zb, slot).wait_send()

            @pl.when(jnp.logical_not(is_home(zb)))
            def _():
                f_copy(zb).wait_send()

            return carry

        lax.fori_loop(0, nz, drain, 0)
        for dist in range(1, nz // 2):
            forward(dist, 0).wait_send()
            if dist < nz // 2 - 1:
                forward(dist, 1).wait_send()

        @pl.when(home)
        def _():
            for k in range(1, pieces_n):
                x2_copy(k).wait_send()

    f32, bf16, i16 = jnp.float32, jnp.bfloat16, jnp.int16
    dma = pltpu.SemaphoreType.DMA
    scratch = [
        pltpu.VMEM((vocab, 2 * depth), bf16),
        pltpu.VMEM((pieces_n, rows, depth + LANES), bf16),
        pltpu.VMEM((pieces_n, rows, depth + LANES), bf16),
        pltpu.VMEM((small, depth + LANES), f32),
        pltpu.VMEM((ny, small, depth + LANES), bf16),
        pltpu.VMEM((block, depth + LANES), f32),
        pltpu.VMEM((nc, nz, block, depth), bf16),
        pltpu.VMEM((nz, 2, block, width), f32),
        pltpu.VMEM((nz, 6, small, width), i16),
        pltpu.VMEM((nz, 2, small, width), i16),
        pltpu.VMEM((nz, 2, 2, small, width), i16),
        pltpu.VMEM((LANES, LANES), f32),
        pltpu.VMEM((nz, 8, LANES), f32),
        pltpu.VMEM((nz, 3, LANES), f32),
        pltpu.VMEM((plane, 3, LANES), f32),
        pltpu.VMEM((8, LANES), f32),
        dma, dma((pieces_n,)), dma((pieces_n,)), dma((2,)), dma((2,)), dma((2,)), dma((2,)),
        dma((nz + 1,)), dma((nz,)), dma((nz,)), dma((nz,)), dma((nz,)), dma((nz,)),
        dma((nz, 6)), dma((nz, 2)), dma((nz, 2, 2)),
        dma((nz,)), dma, dma((pieces_n,)), dma,
    ]
    return kernel, scratch


def body(prefill_hidden, decode_hidden, lm_head, prefill_targets, decode_targets, decode_live):
    nx, nz = lax.axis_size("dp"), lax.axis_size("z")
    ny, nc = lax.axis_size("y"), lax.axis_size("c")
    pre, dec = prefill_hidden.shape[0], decode_hidden.shape[0]
    rows = pre + dec
    width, vocab = lm_head.shape
    kernel, scratch = make_kernel(nx, nz, ny, nc, rows, width // nc, vocab)
    vmem = pl.BlockSpec(memory_space=pltpu.VMEM)
    smem = pl.BlockSpec(memory_space=pltpu.SMEM)
    values = pl.pallas_call(
        kernel,
        out_shape=jax.ShapeDtypeStruct((8, LANES), jnp.float32),
        in_specs=[vmem, vmem, smem, smem, pl.BlockSpec(memory_space=pl.ANY)],
        out_specs=vmem,
        scratch_shapes=scratch,
        compiler_params=pltpu.CompilerParams(
            collective_id=0, has_side_effects=True, vmem_limit_bytes=60 << 20),
    )(prefill_hidden, decode_hidden, prefill_targets, decode_targets, lm_head.T)
    at = (lax.axis_index("dp") * nc + lax.axis_index("c")) * rows
    own = lax.dynamic_slice_in_dim(values[0], at, rows, 0)
    positions = lax.axis_index(VOCAB) * dec + jnp.arange(dec, dtype=jnp.int32)
    decode = jnp.where(positions < decode_live[0], own[pre:], jnp.float32(0.0))
    return own[:pre], decode


def solution(mesh):
    split = Mesh(mesh.devices.reshape(mesh.shape["dp"], 8, 4, 2), DP_VOCAB)
    placed = (
        P(DP_VOCAB, None),
        P(DP_VOCAB, None),
        P("dp", VOCAB),
        P(DP_VOCAB),
        P(DP_VOCAB),
        P("dp"),
    )
    return jax.shard_map(
        body, mesh=split, in_specs=placed, out_specs=(P(DP_VOCAB), P(DP_VOCAB)), check_vma=False
    )
```

```python
import jax
import jax.numpy as jnp
from jax import lax
from jax.experimental import pallas as pl
from jax.experimental.pallas import tpu as pltpu
from jax.sharding import Mesh
from jax.sharding import PartitionSpec as P

VOCAB = ("z", "y", "c")
DP_VOCAB = ("dp", "z", "y", "c")
MESH = pl.DeviceIdType.MESH
LANES = 128
CHUNK = 256
TOP = 32000.0


def make_kernel(nx, nz, ny, nc, rows, n_dec, depth, vocab):
    pieces_n = nx * nc
    small = pieces_n * rows
    block = ny * small
    first_n = vocab // 32 * 16
    counts = (first_n, vocab - first_n)
    width = -(-(max(counts) + 1) // 512) * 512
    plane = nz * ny * nc

    def kernel(pre_hbm, dec_hbm, pt_hbm, dt_hbm, live_hbm, w_hbm, pre_hbm_out, dec_hbm_out,
               pre_ref, dec_ref, pt_ref, dt_ref, live_ref, w, pieces, xrecv, f40, ybuf, fblk, hall, part, sbuf, rel, rd,
               stat, tt, st, fin, res, got, pre_out, dec_out,
               w_sem, in_sem, xs, xr, ys, yr, yf, yfr, ags, agr, d2s, d2r, ts, tr, rs, rlr, rdr,
               fs, fr, x2s, x2r):
        x = lax.axis_index("dp")
        z = lax.axis_index("z")
        y = lax.axis_index("y")
        c = lax.axis_index("c")
        other = 1 - c
        me = x * nc + c
        right = (lax.rem(x + 1, nx), z, y, c)
        left = (lax.rem(x + nx - 1, nx), z, y, c)
        w_copy = pltpu.make_async_copy(w_hbm, w, w_sem)
        w_copy.start()
        inputs = [pltpu.make_async_copy(src, dst, in_sem.at[k]) for k, (src, dst) in enumerate(
            ((pre_hbm, pre_ref), (dec_hbm, dec_ref), (pt_hbm, pt_ref), (dt_hbm, dt_ref),
             (live_hbm, live_ref)))]
        for copy in inputs:
            copy.start()

        def send(src, dst, ssem, rsem, dev):
            return pltpu.make_async_remote_copy(
                src_ref=src, dst_ref=dst, send_sem=ssem, recv_sem=rsem,
                device_id=dev, device_id_type=MESH)

        def arrival(dst, sem):
            return send(dst, dst, sem, sem, (x, z, y, other))

        barrier = pltpu.get_barrier_semaphore()
        peers = []
        for k in range(1, pieces_n):
            p = lax.rem(me + k, pieces_n)
            peers.append((lax.div(p, nc), z, y, lax.rem(p, nc)))
        for k in range(1, ny):
            peers.append((x, z, lax.rem(y + k, ny), c))
        for k in (1, nz - 1):
            peers.append((x, lax.rem(z + k, nz), y, c))
        for dev in peers:
            pl.semaphore_signal(barrier, inc=1, device_id=dev, device_id_type=MESH)

        n_pre = pre_ref.shape[0]
        for copy in inputs:
            copy.wait()
        lane = lax.broadcasted_iota(jnp.int32, (rows, LANES), 1)
        row = lax.broadcasted_iota(jnp.int32, (rows, LANES), 0)
        ids = jnp.zeros((rows, LANES), jnp.int32)
        for r in range(rows):
            ids = jnp.where(row == r, pt_ref[r] if r < n_pre else dt_ref[r - n_pre], ids)
        digits = jnp.where(lane == 0, ids % 256,
                           jnp.where(lane == 1, (ids // 256) % 256,
                                     jnp.where(lane == 2, ids // 65536, 0))).astype(jnp.float32)
        for p in range(pieces_n):
            cols = slice(p * depth, (p + 1) * depth)
            own = jnp.concatenate([pre_ref[:, cols].astype(jnp.float32),
                                   dec_ref[:, cols].astype(jnp.float32)], axis=0)
            pieces[p, :, 0:depth] = own.astype(jnp.bfloat16)
            pieces[p, :, depth:depth + LANES] = digits.astype(jnp.bfloat16)
        for k in range(nz):
            for h in range(2):
                part[k, h, :, width - LANES:width] = jnp.zeros((block, LANES), jnp.float32)
        stat[...] = jnp.zeros(stat.shape, jnp.float32)

        pl.semaphore_wait(barrier, len(peers))

        def x_copy(k):
            p = lax.rem(me + k, pieces_n)
            return send(pieces.at[p], xrecv.at[me], xs.at[p], xr.at[me],
                        (lax.div(p, nc), z, y, lax.rem(p, nc)))

        for k in range(1, pieces_n):
            x_copy(k).start()
        xrecv[me] = pieces[me]
        for k in range(1, pieces_n):
            p = lax.rem(me + k, pieces_n)
            arrival(xrecv.at[p], xr.at[p]).wait_recv()
        for s in range(pieces_n):
            f40[s * rows:(s + 1) * rows, :] = xrecv[s].astype(jnp.float32)

        ybuf[y] = f40[...].astype(jnp.bfloat16)
        up, down = lax.rem(y + 1, ny), lax.rem(y + ny - 1, ny)
        mid = (depth + LANES) // 2

        def y_part(slot, k):
            return ybuf.at[slot, :, pl.ds(k * mid, mid)]

        def y_copy(way, k):
            return send(y_part(y, k), y_part(y, k), ys.at[way, k], yr.at[way, k],
                        (x, z, up if way else down, c))

        def y_forward(way):
            src = y_part(down if way else up, way)
            return send(src, src, yf.at[way], yfr.at[way], (x, z, up if way else down, c))

        for far_half in (True, False):
            for way in (1, 0):
                y_copy(way, way if far_half else 1 - way).start()
        for way in (1, 0):
            arrival(y_part(down if way else up, way), yr.at[way, way]).wait_recv()
            y_forward(way).start()
        far = lax.rem(y + 2, ny)
        for way in (1, 0):
            arrival(y_part(down if way else up, 1 - way), yr.at[way, 1 - way]).wait_recv()
        for way in (1, 0):
            arrival(y_part(far, way), yfr.at[way]).wait_recv()
        for s in range(ny):
            fblk[s * small:(s + 1) * small, :] = ybuf[s].astype(jnp.float32)
        hall[c, z] = fblk[:, 0:depth].astype(jnp.bfloat16)

        def own_copy(way):
            zz = lax.rem(z + (1 if way else nz - 1), nz)
            return send(hall.at[c, z], hall.at[c, z], ags.at[nz if way else z], agr.at[z],
                        (x, zz, y, c))

        def core_copy(zb):
            return send(hall.at[c, zb], hall.at[c, zb], d2s.at[zb], d2r.at[zb], (x, z, y, other))

        own_copy(0).start()
        own_copy(1).start()
        core_copy(z).start()

        digit = lax.broadcasted_iota(jnp.int32, (small, LANES), 1)
        weight = jnp.where(digit == 0, 1.0, jnp.where(digit == 1, 256.0,
                                                      jnp.where(digit == 2, 65536.0, 0.0)))
        at_x = pl.ds(pl.multiple_of(x * small, 8), small)
        named = jnp.sum(fblk[at_x, depth:depth + LANES] * weight, axis=1, keepdims=True)
        stat[0:small, :] = jnp.broadcast_to(named, (small, LANES))
        tt[z] = jnp.transpose(stat[...])[0:8, :]

        def t_copy(k):
            zz = lax.rem(z + k, nz)
            return send(tt.at[z], tt.at[z], ts.at[zz], tr.at[z], (x, zz, y, c))

        w_copy.wait()

        def block_of(i):
            odd = lax.rem(i, 2)
            dist = lax.div(i + 1, 2)
            return lax.rem(z + nz + jnp.where(odd == 1, dist, -dist), nz)

        def forward(dist, way):
            zb = lax.rem(z + nz + (-dist if way else dist), nz)
            zz = lax.rem(z + (1 if way else nz - 1), nz)
            return send(hall.at[c, zb], hall.at[c, zb], ags.at[zb], agr.at[zb], (x, zz, y, c))

        def product(rows_of, columns_of):
            return lax.dot_general(rows_of, columns_of, (((1,), (1,)), ((), ())),
                                   preferred_element_type=jnp.float32)

        def multiply(blocks, h):
            base = h * first_n
            for n0 in range(0, counts[h], 512):
                n1 = min(n0 + 512, counts[h])
                at = slice(base + n0, base + n1)
                lhs = [jnp.concatenate([hall[k, zb] for zb in blocks], axis=0)
                       if len(blocks) > 1 else hall[k, blocks[0]] for k in range(2)]
                acc = product(lhs[0], w[at, 0:depth]) + product(lhs[1], w[at, depth:2 * depth])
                for j, zb in enumerate(blocks):
                    part[zb, h, :, n0:n1] = acc[j * block:(j + 1) * block]

        def rows_at(q):
            return pl.ds(pl.multiple_of(q * small, 8), small)

        def step_of(code, h):
            return jnp.exp2(code[:, LANES - 1:LANES].astype(jnp.int32).astype(jnp.float32))

        def unpack(code, n0, h, step):
            v = code.astype(jnp.int32).astype(jnp.float32) * step
            if n0 + CHUNK > counts[h]:
                col = lax.broadcasted_iota(jnp.int32, v.shape, 1)
                v = jnp.where(col >= counts[h] - n0, 0.0, v)
            return v

        def quantise(zb, h, q, slot, relayed):
            at = rows_at(q)
            big = jnp.zeros((small, LANES), jnp.float32)
            if relayed:
                step = step_of(rel[zb, h, :, width - LANES:width], h)
            for n0 in range(0, width, CHUNK):
                v = part[zb, h, at, n0:n0 + CHUNK]
                if relayed:
                    v = v + unpack(rel[zb, h, :, n0:n0 + CHUNK], n0, h, step)
                    part[zb, h, at, n0:n0 + CHUNK] = v
                for k in range(0, CHUNK, LANES):
                    big = jnp.maximum(big, jnp.abs(v[:, k:k + LANES]))
            big = jnp.max(big, axis=1, keepdims=True)
            e = jnp.ceil(jnp.log2(jnp.maximum(big, 1e-20) * (1.0 / TOP)))
            scale = jnp.exp2(-e)
            for n0 in range(0, width, CHUNK):
                v = jnp.round(part[zb, h, at, n0:n0 + CHUNK] * scale)
                if n0 + CHUNK > counts[h]:
                    col = lax.broadcasted_iota(jnp.int32, v.shape, 1)
                    v = jnp.where(col >= counts[h] - n0, e, v)
                sbuf[zb, slot, :, n0:n0 + CHUNK] = v.astype(jnp.int32).astype(jnp.int16)

        toward_left = lax.rem(x + nx - 1, nx)
        toward_right = lax.rem(x + 1, nx)
        opposite = lax.rem(x + 2, nx)

        def message(zb, slot):
            if slot == 0:
                dst, rsem, dev = rel.at[zb, 0], rlr.at[zb, 0], left
            elif slot == 1:
                dst, rsem, dev = rel.at[zb, 1], rlr.at[zb, 1], right
            elif slot in (2, 4):
                h = 1 if slot == 2 else 0
                dst, rsem, dev = rd.at[zb, 0, h], rdr.at[zb, 0, h], left
            else:
                h = 0 if slot == 3 else 1
                dst, rsem, dev = rd.at[zb, 1, h], rdr.at[zb, 1, h], right
            return send(sbuf.at[zb, slot], dst, rs.at[zb, slot], rsem, dev)

        def emit(zb, h, slots):
            for slot in slots:
                quantise(zb, h, {2: toward_left, 3: toward_right}.get(slot, opposite), slot, False)
                message(zb, slot).start()

        def pass_on(zb):
            arrival(rel.at[zb, 0], rlr.at[zb, 0]).wait_recv()
            quantise(zb, 0, toward_left, 4, True)
            message(zb, 4).start()
            arrival(rel.at[zb, 1], rlr.at[zb, 1]).wait_recv()
            quantise(zb, 1, toward_right, 5, True)
            message(zb, 5).start()

        def pass_pair(dist):
            def one(j, carry):
                pass_on(lax.rem(z + nz + jnp.where(j == 0, dist, -dist), nz))
                return carry

            lax.fori_loop(0, 2, one, 0)

        arrival(hall.at[other, z], d2r.at[z]).wait_recv()
        for h in range(2):
            multiply([z], h)
            emit(z, h, (h, 3 - h))

        def pair(dist, carry):
            above = lax.rem(z + dist, nz)
            below = lax.rem(z + nz - dist, nz)
            arrival(hall.at[c, above], agr.at[above]).wait_recv()
            core_copy(above).start()
            forward(dist, 0).start()
            arrival(hall.at[c, below], agr.at[below]).wait_recv()
            core_copy(below).start()

            @pl.when(dist < nz // 2 - 1)
            def _():
                forward(dist, 1).start()

            t_copy(dist).start()
            t_copy(nz - dist).start()

            @pl.when(dist == 1)
            def _():
                pass_on(z)

            arrival(hall.at[other, above], d2r.at[above]).wait_recv()
            arrival(hall.at[other, below], d2r.at[below]).wait_recv()
            for h in range(2):
                multiply([above, below], h)

                def one(j, carry):
                    emit(jnp.where(j == 0, above, below), h, (h, 3 - h))
                    return carry

                lax.fori_loop(0, 2, one, 0)
                if h == 0:
                    @pl.when(dist > 1)
                    def _():
                        pass_pair(dist - 1)

            return carry

        lax.fori_loop(1, nz // 2, pair, 0)
        across = lax.rem(z + nz // 2, nz)
        arrival(hall.at[c, across], agr.at[across]).wait_recv()
        core_copy(across).start()
        t_copy(nz // 2).start()
        arrival(hall.at[other, across], d2r.at[across]).wait_recv()
        for h in range(2):
            multiply([across], h)
            emit(across, h, (h,))
        pass_pair(nz // 2 - 1)
        for h in range(2):
            emit(across, h, (3 - h,))

        first = (((z * ny + y) * nc + c) * vocab).astype(jnp.float32)
        mine = (z * ny + y) * nc + c
        at_row = rows_at(x)

        def home_of(zb):
            return (x, zb, x, lax.div(zb * nc, nz))

        def f_copy(zb):
            return send(st.at[zb], fin.at[mine], fs.at[zb], fr, home_of(zb))

        def is_home(zb):
            return jnp.logical_and(jnp.logical_and(z == zb, y == x), c == lax.div(zb * nc, nz))

        def reduce(i, carry):
            zb = block_of(i)

            @pl.when(zb != z)
            def _():
                arrival(tt.at[zb], tr.at[zb]).wait_recv()

            wanted = jnp.transpose(jnp.broadcast_to(tt[zb, 0:1, :], (LANES, LANES)))[0:small, 0:1]
            big = jnp.full((small, LANES), -jnp.inf, jnp.float32)
            picked = jnp.zeros((small, LANES), jnp.float32)
            for h in range(2):
                for side in range(2):
                    arrival(rd.at[zb, side, h], rdr.at[zb, side, h]).wait_recv()
                steps = [step_of(rd[zb, side, h, :, width - LANES:width], h) for side in range(2)]
                local = (wanted - (first + float(h * first_n))).astype(jnp.int32)
                local = jnp.where(jnp.logical_and(local >= 0, local < counts[h]), local, -1)
                for n0 in range(0, width, CHUNK):
                    at = slice(n0, n0 + CHUNK)
                    v = part[zb, h, at_row, at] + (unpack(rd[zb, 0, h, :, at], n0, h, steps[0])
                                                   + unpack(rd[zb, 1, h, :, at], n0, h, steps[1]))
                    col = lax.broadcasted_iota(jnp.int32, v.shape, 1)
                    hit = jnp.where(col == local - n0, v, 0.0)
                    if n0 + CHUNK > counts[h]:
                        v = jnp.where(col >= counts[h] - n0, -jnp.inf, v)
                    part[zb, h, at_row, at] = v
                    for k in range(0, CHUNK, LANES):
                        big = jnp.maximum(big, v[:, k:k + LANES])
                        picked = picked + hit[:, k:k + LANES]
            top = jnp.max(big, axis=1, keepdims=True)
            total = jnp.zeros((small, LANES), jnp.float32)
            for h in range(2):
                for n0 in range(0, width, CHUNK):
                    v = jnp.exp(part[zb, h, at_row, n0:n0 + CHUNK] - top)
                    for k in range(0, CHUNK, LANES):
                        total = total + v[:, k:k + LANES]
            total = jnp.sum(total, axis=1, keepdims=True)
            picked = jnp.sum(picked, axis=1, keepdims=True)
            ln = lax.broadcasted_iota(jnp.int32, (small, LANES), 1)
            stat[0:small, :] = jnp.where(ln == 0, top, jnp.where(ln == 1, total,
                                                                jnp.where(ln == 2, picked, 0.0)))
            tile = jnp.transpose(stat[...])[0:3, :]
            st[zb] = tile

            @pl.when(is_home(zb))
            def _():
                fin[mine] = tile

            @pl.when(jnp.logical_not(is_home(zb)))
            def _():
                f_copy(zb).start()

            return carry

        early = nz - 3
        lax.fori_loop(0, early, reduce, 0)
        pass_on(across)
        lax.fori_loop(early, nz, reduce, 0)
        for k in range(1, pieces_n):
            x_copy(k).wait_send()
        for way in range(2):
            for k in range(2):
                y_copy(way, k).wait_send()
            y_forward(way).wait_send()
            own_copy(way).wait_send()
        for k in range(1, nz):
            t_copy(k).wait_send()

        def drain(i, carry):
            zb = block_of(i)
            core_copy(zb).wait_send()
            for slot in range(6):
                message(zb, slot).wait_send()

            @pl.when(jnp.logical_not(is_home(zb)))
            def _():
                f_copy(zb).wait_send()

            return carry

        lax.fori_loop(0, nz, drain, 0)
        for dist in range(1, nz // 2):
            forward(dist, 0).wait_send()
            if dist < nz // 2 - 1:
                forward(dist, 1).wait_send()

        home = is_home(z)

        def x2_copy(k):
            p = lax.rem(me + k, pieces_n)
            return send(res, got, x2s.at[p], x2r, (lax.div(p, nc), z, y, lax.rem(p, nc)))

        @pl.when(home)
        def _():
            arrival(fin.at[0:plane - 1], fr).wait_recv()
            tops = fin[:, 0, :]
            top = jnp.max(tops, axis=0, keepdims=True)
            total = jnp.sum(fin[:, 1, :] * jnp.exp(tops - top), axis=0, keepdims=True)
            picked = jnp.sum(fin[:, 2, :], axis=0, keepdims=True)
            value = jnp.broadcast_to(picked - (top + jnp.log(total)), (8, LANES))
            res[...] = value
            for k in range(1, pieces_n):
                x2_copy(k).start()
            got[...] = value

        @pl.when(jnp.logical_not(home))
        def _():
            arrival(got, x2r).wait_recv()

        values = pltpu.roll(got[...], LANES - me * rows, 1)
        lanes = lax.broadcasted_iota(jnp.int32, (8, LANES), 1)
        position = mine * n_dec + lanes - n_pre
        values = jnp.where(jnp.logical_and(lanes >= n_pre, position >= live_ref[0]), 0.0, values)
        pre_out[...] = values[0, 0:n_pre]
        dec_out[...] = values[0, n_pre:rows]
        outputs = [pltpu.make_async_copy(pre_out, pre_hbm_out, in_sem.at[0]),
                   pltpu.make_async_copy(dec_out, dec_hbm_out, in_sem.at[1])]
        for copy in outputs:
            copy.start()

        @pl.when(home)
        def _():
            for k in range(1, pieces_n):
                x2_copy(k).wait_send()

        for copy in outputs:
            copy.wait()

    f32, bf16, i16 = jnp.float32, jnp.bfloat16, jnp.int16
    dma = pltpu.SemaphoreType.DMA
    scratch = [
        pltpu.VMEM((rows - n_dec, nx * nc * depth), bf16),
        pltpu.VMEM((n_dec, nx * nc * depth), bf16),
        pltpu.SMEM((rows - n_dec,), jnp.int32),
        pltpu.SMEM((n_dec,), jnp.int32),
        pltpu.SMEM((1,), jnp.int32),
        pltpu.VMEM((vocab, 2 * depth), bf16),
        pltpu.VMEM((pieces_n, rows, depth + LANES), bf16),
        pltpu.VMEM((pieces_n, rows, depth + LANES), bf16),
        pltpu.VMEM((small, depth + LANES), f32),
        pltpu.VMEM((ny, small, depth + LANES), bf16),
        pltpu.VMEM((block, depth + LANES), f32),
        pltpu.VMEM((nc, nz, block, depth), bf16),
        pltpu.VMEM((nz, 2, block, width), f32),
        pltpu.VMEM((nz, 6, small, width), i16),
        pltpu.VMEM((nz, 2, small, width), i16),
        pltpu.VMEM((nz, 2, 2, small, width), i16),
        pltpu.VMEM((LANES, LANES), f32),
        pltpu.VMEM((nz, 8, LANES), f32),
        pltpu.VMEM((nz, 3, LANES), f32),
        pltpu.VMEM((plane, 3, LANES), f32),
        pltpu.VMEM((8, LANES), f32),
        pltpu.VMEM((8, LANES), f32),
        pltpu.VMEM((rows - n_dec,), f32),
        pltpu.VMEM((n_dec,), f32),
        dma, dma((5,)), dma((pieces_n,)), dma((pieces_n,)), dma((2, 2)), dma((2, 2)), dma((2,)), dma((2,)),
        dma((nz + 1,)), dma((nz,)), dma((nz,)), dma((nz,)), dma((nz,)), dma((nz,)),
        dma((nz, 6)), dma((nz, 2)), dma((nz, 2, 2)),
        dma((nz,)), dma, dma((pieces_n,)), dma,
    ]
    return kernel, scratch


def body(prefill_hidden, decode_hidden, lm_head, prefill_targets, decode_targets, decode_live):
    nx, nz = lax.axis_size("dp"), lax.axis_size("z")
    ny, nc = lax.axis_size("y"), lax.axis_size("c")
    pre, dec = prefill_hidden.shape[0], decode_hidden.shape[0]
    rows = pre + dec
    width, vocab = lm_head.shape
    kernel, scratch = make_kernel(nx, nz, ny, nc, rows, dec, width // nc, vocab)
    hbm = pl.BlockSpec(memory_space=pltpu.HBM)
    return pl.pallas_call(
        kernel,
        out_shape=(jax.ShapeDtypeStruct((pre,), jnp.float32),
                   jax.ShapeDtypeStruct((dec,), jnp.float32)),
        in_specs=[hbm] * 6,
        out_specs=(hbm, hbm),
        scratch_shapes=scratch,
        compiler_params=pltpu.CompilerParams(
            collective_id=0, has_side_effects=True, vmem_limit_bytes=60 << 20),
    )(prefill_hidden, decode_hidden, prefill_targets, decode_targets, decode_live, lm_head.T)


def solution(mesh):
    split = Mesh(mesh.devices.reshape(mesh.shape["dp"], 8, 4, 2), DP_VOCAB)
    placed = (
        P(DP_VOCAB, None),
        P(DP_VOCAB, None),
        P("dp", VOCAB),
        P(DP_VOCAB),
        P(DP_VOCAB),
        P("dp"),
    )
    return jax.shard_map(
        body, mesh=split, in_specs=placed, out_specs=(P(DP_VOCAB), P(DP_VOCAB)), check_vma=False
    )
```

```python
import jax
import jax.numpy as jnp
from jax import lax
from jax.experimental import pallas as pl
from jax.experimental.pallas import tpu as pltpu
from jax.sharding import Mesh
from jax.sharding import PartitionSpec as P

VOCAB = ("z", "y", "c")
DP_VOCAB = ("dp", "z", "y", "c")
MESH = pl.DeviceIdType.MESH
LANES = 128
CHUNK = 256
TOP = 32000.0


def make_kernel(nx, nz, ny, nc, rows, n_dec, depth, vocab):
    pieces_n = nx * nc
    small = pieces_n * rows
    block = ny * small
    first_n = vocab // 32 * 16
    counts = (first_n, vocab - first_n)
    width = -(-(max(counts) + 1) // 512) * 512
    plane = nz * ny * nc

    def kernel(pre_hbm, dec_hbm, pt_hbm, dt_hbm, live_hbm, w_hbm, pre_hbm_out, dec_hbm_out,
               pre_ref, dec_ref, pt_ref, dt_ref, live_ref, w, pieces, xrecv, f40, ybuf, hall, dense, part, sbuf, rel, rd,
               stat, tt, st, fin, res, got, pre_out, dec_out,
               w_sem, in_sem, xs, xr, ys, yr, yf, yfr, ags, agr, d2s, d2r, ts, tr, rs, rlr, rdr,
               fs, fr, x2s, x2r):
        x = lax.axis_index("dp")
        z = lax.axis_index("z")
        y = lax.axis_index("y")
        c = lax.axis_index("c")
        other = 1 - c
        me = x * nc + c
        x_up = (lax.rem(x + 1, nx), z, y, c)
        x_down = (lax.rem(x + nx - 1, nx), z, y, c)
        w_copy = pltpu.make_async_copy(w_hbm, w, w_sem)
        w_copy.start()
        inputs = [pltpu.make_async_copy(src, dst, in_sem.at[k]) for k, (src, dst) in enumerate(
            ((pre_hbm, pre_ref), (dec_hbm, dec_ref), (pt_hbm, pt_ref), (dt_hbm, dt_ref),
             (live_hbm, live_ref)))]
        for copy in inputs:
            copy.start()

        def send(src, dst, ssem, rsem, dev):
            return pltpu.make_async_remote_copy(
                src_ref=src, dst_ref=dst, send_sem=ssem, recv_sem=rsem,
                device_id=dev, device_id_type=MESH)

        def arrival(dst, sem):
            return send(dst, dst, sem, sem, (x, z, y, other))

        barrier = pltpu.get_barrier_semaphore()
        peers = []
        for k in range(1, pieces_n):
            p = lax.rem(me + k, pieces_n)
            peers.append((lax.div(p, nc), z, y, lax.rem(p, nc)))
        for k in range(1, ny):
            peers.append((x, z, lax.rem(y + k, ny), c))
        for k in (1, nz - 1):
            peers.append((x, lax.rem(z + k, nz), y, c))
        for dev in peers:
            pl.semaphore_signal(barrier, inc=1, device_id=dev, device_id_type=MESH)

        n_pre = pre_ref.shape[0]
        for copy in inputs:
            copy.wait()
        lane = lax.broadcasted_iota(jnp.int32, (rows, LANES), 1)
        row = lax.broadcasted_iota(jnp.int32, (rows, LANES), 0)
        ids = jnp.zeros((rows, LANES), jnp.int32)
        for r in range(rows):
            ids = jnp.where(row == r, pt_ref[r] if r < n_pre else dt_ref[r - n_pre], ids)
        digits = jnp.where(lane == 0, ids % 256,
                           jnp.where(lane == 1, (ids // 256) % 256,
                                     jnp.where(lane == 2, ids // 65536, 0))).astype(jnp.float32)
        for p in range(pieces_n):
            cols = slice(p * depth, (p + 1) * depth)
            own = jnp.concatenate([pre_ref[:, cols].astype(jnp.float32),
                                   dec_ref[:, cols].astype(jnp.float32)], axis=0)
            pieces[p, :, 0:depth] = own.astype(jnp.bfloat16)
            pieces[p, :, depth:depth + LANES] = digits.astype(jnp.bfloat16)
        for k in range(nz):
            for h in range(2):
                part[k, h, :, width - LANES:width] = jnp.zeros((block, LANES), jnp.float32)
        stat[...] = jnp.zeros(stat.shape, jnp.float32)

        pl.semaphore_wait(barrier, len(peers))

        def x_copy(k):
            p = lax.rem(me + k, pieces_n)
            return send(pieces.at[p], xrecv.at[me], xs, xr,
                        (lax.div(p, nc), z, y, lax.rem(p, nc)))

        for k in range(1, pieces_n):
            x_copy(k).start()
        xrecv[me] = pieces[me]
        arrival(xrecv.at[0:pieces_n - 1], xr).wait_recv()
        for s in range(pieces_n):
            f40[s * rows:(s + 1) * rows, :] = xrecv[s].astype(jnp.float32)

        ybuf[y] = f40[...].astype(jnp.bfloat16)
        up, down = lax.rem(y + 1, ny), lax.rem(y + ny - 1, ny)
        mid = (depth + LANES) // 2

        def y_part(slot, k):
            return ybuf.at[slot, :, pl.ds(k * mid, mid)]

        def y_copy(way, k):
            return send(y_part(y, k), y_part(y, k), ys, yr.at[way, k],
                        (x, z, up if way else down, c))

        def y_forward(way):
            src = y_part(down if way else up, way)
            return send(src, src, yf, yfr.at[way], (x, z, up if way else down, c))

        above_z, below_z = lax.rem(z + 1, nz), lax.rem(z + nz - 1, nz)

        def spread(j):
            src = ybuf.at[j, :, pl.ds(0, depth)]
            for zz in (above_z, below_z):
                send(src, hall.at[c, z, j], ags, agr.at[z, j], (x, zz, y, c)).start()
            send(src, hall.at[c, z, j], d2s, d2r.at[z], (x, z, y, other)).start()
            hall[c, z, j] = ybuf[j, :, 0:depth]

        def take(dist, parts):
            up_zb, down_zb = lax.rem(z + dist, nz), lax.rem(z + nz - dist, nz)

            def ring(zb, j, zz):
                return send(hall.at[c, zb, j], hall.at[c, zb, j], ags, agr.at[zb, j],
                            (x, zz, y, c))

            def got_rows(zb, j):
                arrival(hall.at[c, zb, j], agr.at[zb, j]).wait_recv()

            def core_copy(zb, j):
                return send(hall.at[c, zb, j], hall.at[c, zb, j], d2s, d2r.at[zb],
                            (x, z, y, other))

            for j in parts:
                got_rows(up_zb, j)

                @pl.when(dist < nz // 2)
                def _():
                    ring(up_zb, j, below_z).start()
                    got_rows(down_zb, j)

                @pl.when(dist < nz // 2 - 1)
                def _():
                    ring(down_zb, j, above_z).start()

                core_copy(up_zb, j).start()

                @pl.when(dist < nz // 2)
                def _():
                    core_copy(down_zb, j).start()

        for far_half in (True, False):
            for way in (1, 0):
                y_copy(way, way if far_half else 1 - way).start()
        spread(y)
        for way in (1, 0):
            arrival(y_part(down if way else up, way), yr.at[way, way]).wait_recv()
            y_forward(way).start()
        for way in (1, 0):
            arrival(y_part(down if way else up, 1 - way), yr.at[way, 1 - way]).wait_recv()
            spread(down if way else up)
        far = lax.rem(y + 2, ny)
        for way in (1, 0):
            arrival(y_part(far, way), yfr.at[way]).wait_recv()
        spread(far)
        one_hop = z * 0 + 1
        take(one_hop, (y,))

        digit = lax.broadcasted_iota(jnp.int32, (small, LANES), 1)
        weight = jnp.where(digit == 0, 1.0, jnp.where(digit == 1, 256.0,
                                                      jnp.where(digit == 2, 65536.0, 0.0)))
        mine_digits = ybuf[x, :, depth:depth + LANES].astype(jnp.float32)
        named = jnp.sum(mine_digits * weight, axis=1, keepdims=True)
        stat[0:small, :] = jnp.broadcast_to(named, (small, LANES))
        tt[z] = jnp.transpose(stat[...])[0:8, :]

        def t_copy(k):
            zz = lax.rem(z + k, nz)
            return send(tt.at[z], tt.at[z], ts, tr, (x, zz, y, c))

        w_copy.wait()

        def block_of(i):
            odd = lax.rem(i, 2)
            dist = lax.div(i + 1, 2)
            return lax.rem(z + nz + jnp.where(odd == 1, dist, -dist), nz)

        def product(rows_of, columns_of):
            return lax.dot_general(rows_of, columns_of, (((1,), (1,)), ((), ())),
                                   preferred_element_type=jnp.float32)

        def align(blocks):
            for k in range(2):
                for c0 in range(0, depth, LANES):
                    rows_of = jnp.concatenate([hall[k, zb, j, :, c0:c0 + LANES].astype(jnp.float32)
                                               for zb in blocks for j in range(ny)], axis=0)
                    dense[k, 0:len(blocks) * block, c0:c0 + LANES] = rows_of.astype(jnp.bfloat16)

        def multiply(blocks, h):
            base = h * first_n
            n_rows = len(blocks) * block
            for n0 in range(0, counts[h], 512):
                n1 = min(n0 + 512, counts[h])
                at = slice(base + n0, base + n1)
                acc = (product(dense[0, 0:n_rows], w[at, 0:depth])
                       + product(dense[1, 0:n_rows], w[at, depth:2 * depth]))
                for j, zb in enumerate(blocks):
                    part[zb, h, :, n0:n1] = acc[j * block:(j + 1) * block]

        def rows_at(q):
            return pl.ds(pl.multiple_of(q * small, 8), small)

        def step_of(code, h):
            return jnp.exp2(code[:, LANES - 1:LANES].astype(jnp.int32).astype(jnp.float32))

        def unpack(code, n0, h, step):
            v = code.astype(jnp.int32).astype(jnp.float32) * step
            if n0 + CHUNK > counts[h]:
                col = lax.broadcasted_iota(jnp.int32, v.shape, 1)
                v = jnp.where(col >= counts[h] - n0, 0.0, v)
            return v

        def quantise(zb, h, q, slot, relayed):
            at = rows_at(q)
            big = jnp.zeros((small, LANES), jnp.float32)
            if relayed:
                step = step_of(rel[zb, h, :, width - LANES:width], h)
            for n0 in range(0, width, CHUNK):
                v = part[zb, h, at, n0:n0 + CHUNK]
                if relayed:
                    v = v + unpack(rel[zb, h, :, n0:n0 + CHUNK], n0, h, step)
                    part[zb, h, at, n0:n0 + CHUNK] = v
                for k in range(0, CHUNK, LANES):
                    big = jnp.maximum(big, jnp.abs(v[:, k:k + LANES]))
            big = jnp.max(big, axis=1, keepdims=True)
            e = jnp.ceil(jnp.log2(jnp.maximum(big, 1e-20) * (1.0 / TOP)))
            scale = jnp.exp2(-e)
            for n0 in range(0, width, CHUNK):
                v = jnp.round(part[zb, h, at, n0:n0 + CHUNK] * scale)
                if n0 + CHUNK > counts[h]:
                    col = lax.broadcasted_iota(jnp.int32, v.shape, 1)
                    v = jnp.where(col >= counts[h] - n0, e, v)
                sbuf[zb, slot, :, n0:n0 + CHUNK] = v.astype(jnp.int32).astype(jnp.int16)

        toward_left = lax.rem(x + nx - 1, nx)
        toward_right = lax.rem(x + 1, nx)
        opposite = lax.rem(x + 2, nx)

        def message(zb, slot):
            if slot == 0:
                dst, rsem, dev = rel.at[zb, 0], rlr.at[zb, 0], x_down
            elif slot == 1:
                dst, rsem, dev = rel.at[zb, 1], rlr.at[zb, 1], x_up
            elif slot in (2, 4):
                h = 1 if slot == 2 else 0
                dst, rsem, dev = rd.at[zb, 0, h], rdr.at[zb], x_down
            else:
                h = 0 if slot == 3 else 1
                dst, rsem, dev = rd.at[zb, 1, h], rdr.at[zb], x_up
            return send(sbuf.at[zb, slot], dst, rs, rsem, dev)

        def emit(zb, h, slots):
            for slot in slots:
                quantise(zb, h, {2: toward_left, 3: toward_right}.get(slot, opposite), slot, False)
                message(zb, slot).start()

        def pass_on(zb):
            arrival(rel.at[zb, 0], rlr.at[zb, 0]).wait_recv()
            quantise(zb, 0, toward_left, 4, True)
            message(zb, 4).start()
            arrival(rel.at[zb, 1], rlr.at[zb, 1]).wait_recv()
            quantise(zb, 1, toward_right, 5, True)
            message(zb, 5).start()

        def pass_pair(dist):
            def one(j, carry):
                pass_on(lax.rem(z + nz + jnp.where(j == 0, dist, -dist), nz))
                return carry

            lax.fori_loop(0, 2, one, 0)

        arrival(hall.at[other, z], d2r.at[z]).wait_recv()
        for h in range(2):
            if h == 0:
                align([z])
            multiply([z], h)
            emit(z, h, (h, 3 - h))
            take(one_hop, (up, down) if h == 0 else (far,))

        def pair(dist, carry):
            above = lax.rem(z + dist, nz)
            below = lax.rem(z + nz - dist, nz)
            t_copy(dist).start()
            t_copy(nz - dist).start()

            arrival(hall.at[other, above], d2r.at[above]).wait_recv()
            arrival(hall.at[other, below], d2r.at[below]).wait_recv()
            for h in range(2):
                if h == 0:
                    align([above, below])
                multiply([above, below], h)

                def one(j, carry):
                    zb = jnp.where(j == 0, above, below)
                    emit(zb, h, (h,))

                    @pl.when(dist > 1)
                    def _():
                        emit(zb, h, (3 - h,))

                    return carry

                lax.fori_loop(0, 2, one, 0)
                take(dist + 1, (y, up) if h == 0 else (down, far))
                if h == 0:
                    @pl.when(dist == 1)
                    def _():
                        pass_on(z)

                    @pl.when(dist > 1)
                    def _():
                        pass_pair(dist - 1)

            return carry

        lax.fori_loop(1, nz // 2, pair, 0)
        across = lax.rem(z + nz // 2, nz)
        t_copy(nz // 2).start()
        arrival(hall.at[other, across], d2r.at[across]).wait_recv()
        for h in range(2):
            if h == 0:
                align([across])
            multiply([across], h)
            emit(across, h, (h,))
        pass_pair(nz // 2 - 1)
        for h in range(2):
            emit(across, h, (3 - h,))

        first = (((z * ny + y) * nc + c) * vocab).astype(jnp.float32)
        mine = (z * ny + y) * nc + c
        at_row = rows_at(x)

        def home_of(zb):
            return (x, zb, x, lax.div(zb * nc, nz))

        def f_copy(zb):
            return send(st.at[zb], fin.at[mine], fs, fr, home_of(zb))

        def is_home(zb):
            return jnp.logical_and(jnp.logical_and(z == zb, y == x), c == lax.div(zb * nc, nz))

        def reduce(i, carry):
            zb = block_of(i)
            arrival(rd.at[zb], rdr.at[zb]).wait_recv()
            wanted = jnp.transpose(jnp.broadcast_to(tt[zb, 0:1, :], (LANES, LANES)))[0:small, 0:1]
            big = jnp.full((small, LANES), -jnp.inf, jnp.float32)
            picked = jnp.zeros((small, LANES), jnp.float32)
            for h in range(2):
                steps = [step_of(rd[zb, side, h, :, width - LANES:width], h) for side in range(2)]
                local = (wanted - (first + float(h * first_n))).astype(jnp.int32)
                local = jnp.where(jnp.logical_and(local >= 0, local < counts[h]), local, -1)
                for n0 in range(0, width, CHUNK):
                    at = slice(n0, n0 + CHUNK)
                    v = part[zb, h, at_row, at] + (unpack(rd[zb, 0, h, :, at], n0, h, steps[0])
                                                   + unpack(rd[zb, 1, h, :, at], n0, h, steps[1]))
                    col = lax.broadcasted_iota(jnp.int32, v.shape, 1)
                    hit = jnp.where(col == local - n0, v, 0.0)
                    if n0 + CHUNK > counts[h]:
                        v = jnp.where(col >= counts[h] - n0, -jnp.inf, v)
                    part[zb, h, at_row, at] = v
                    for k in range(0, CHUNK, LANES):
                        big = jnp.maximum(big, v[:, k:k + LANES])
                        picked = picked + hit[:, k:k + LANES]
            top = jnp.max(big, axis=1, keepdims=True)
            total = jnp.zeros((small, LANES), jnp.float32)
            for h in range(2):
                for n0 in range(0, width, CHUNK):
                    v = jnp.exp(part[zb, h, at_row, n0:n0 + CHUNK] - top)
                    for k in range(0, CHUNK, LANES):
                        total = total + v[:, k:k + LANES]
            total = jnp.sum(total, axis=1, keepdims=True)
            picked = jnp.sum(picked, axis=1, keepdims=True)
            ln = lax.broadcasted_iota(jnp.int32, (small, LANES), 1)
            stat[0:small, :] = jnp.where(ln == 0, top, jnp.where(ln == 1, total,
                                                                jnp.where(ln == 2, picked, 0.0)))
            tile = jnp.transpose(stat[...])[0:3, :]
            st[zb] = tile

            @pl.when(is_home(zb))
            def _():
                fin[mine] = tile

            @pl.when(jnp.logical_not(is_home(zb)))
            def _():
                f_copy(zb).start()

            return carry

        arrival(tt.at[0:nz - 1], tr).wait_recv()
        reduce(0, 0)
        lax.fori_loop(3, nz - 2, reduce, 0)
        pass_on(across)

        def near(j, carry):
            zb = block_of(j)
            for h in range(2):
                emit(zb, h, (3 - h,))
            return carry

        lax.fori_loop(1, 3, near, 0)
        lax.fori_loop(nz - 2, nz, reduce, 0)
        lax.fori_loop(1, 3, reduce, 0)
        def left(ref, sem):
            send(ref, ref, sem, sem, (x, z, y, other)).wait_send()

        home = is_home(z)
        left(pieces.at[0:pieces_n - 1], xs)
        left(ybuf.at[0:2], ys)
        left(ybuf.at[0], yf)
        left(hall.at[c, 0:nz - 1], ags)
        left(hall.at[c], d2s)
        left(tt.at[0:nz - 1], ts)
        left(sbuf, rs)

        @pl.when(home)
        def _():
            left(st.at[0:nz - 1], fs)

        @pl.when(jnp.logical_not(home))
        def _():
            left(st, fs)

        def x2_copy(k):
            p = lax.rem(me + k, pieces_n)
            return send(res, got, x2s, x2r, (lax.div(p, nc), z, y, lax.rem(p, nc)))

        @pl.when(home)
        def _():
            arrival(fin.at[0:plane - 1], fr).wait_recv()
            tops = fin[:, 0, :]
            top = jnp.max(tops, axis=0, keepdims=True)
            total = jnp.sum(fin[:, 1, :] * jnp.exp(tops - top), axis=0, keepdims=True)
            picked = jnp.sum(fin[:, 2, :], axis=0, keepdims=True)
            value = jnp.broadcast_to(picked - (top + jnp.log(total)), (8, LANES))
            res[...] = value
            for k in range(1, pieces_n):
                x2_copy(k).start()
            got[...] = value

        @pl.when(jnp.logical_not(home))
        def _():
            arrival(got, x2r).wait_recv()

        values = pltpu.roll(got[...], LANES - me * rows, 1)
        lanes = lax.broadcasted_iota(jnp.int32, (8, LANES), 1)
        position = mine * n_dec + lanes - n_pre
        values = jnp.where(jnp.logical_and(lanes >= n_pre, position >= live_ref[0]), 0.0, values)
        pre_out[...] = values[0, 0:n_pre]
        dec_out[...] = values[0, n_pre:rows]
        outputs = [pltpu.make_async_copy(pre_out, pre_hbm_out, in_sem.at[0]),
                   pltpu.make_async_copy(dec_out, dec_hbm_out, in_sem.at[1])]
        for copy in outputs:
            copy.start()

        @pl.when(home)
        def _():
            left(tt.at[0:pieces_n - 1], x2s)

        for copy in outputs:
            copy.wait()

    f32, bf16, i16 = jnp.float32, jnp.bfloat16, jnp.int16
    dma = pltpu.SemaphoreType.DMA
    scratch = [
        pltpu.VMEM((rows - n_dec, nx * nc * depth), bf16),
        pltpu.VMEM((n_dec, nx * nc * depth), bf16),
        pltpu.SMEM((rows - n_dec,), jnp.int32),
        pltpu.SMEM((n_dec,), jnp.int32),
        pltpu.SMEM((1,), jnp.int32),
        pltpu.VMEM((vocab, 2 * depth), bf16),
        pltpu.VMEM((pieces_n, rows, depth + LANES), bf16),
        pltpu.VMEM((pieces_n, rows, depth + LANES), bf16),
        pltpu.VMEM((small, depth + LANES), f32),
        pltpu.VMEM((ny, small, depth + LANES), bf16),
        pltpu.VMEM((nc, nz, ny, small, depth), bf16),
        pltpu.VMEM((2, 2 * block, depth), bf16),
        pltpu.VMEM((nz, 2, block, width), f32),
        pltpu.VMEM((nz, 6, small, width), i16),
        pltpu.VMEM((nz, 2, small, width), i16),
        pltpu.VMEM((nz, 2, 2, small, width), i16),
        pltpu.VMEM((LANES, LANES), f32),
        pltpu.VMEM((nz, 8, LANES), f32),
        pltpu.VMEM((nz, 3, LANES), f32),
        pltpu.VMEM((plane, 3, LANES), f32),
        pltpu.VMEM((8, LANES), f32),
        pltpu.VMEM((8, LANES), f32),
        pltpu.VMEM((rows - n_dec,), f32),
        pltpu.VMEM((n_dec,), f32),
        dma, dma((5,)), dma, dma, dma, dma((2, 2)), dma, dma((2,)),
        dma, dma((nz, ny)), dma, dma((nz,)), dma, dma,
        dma, dma((nz, 2)), dma((nz,)),
        dma, dma, dma, dma,
    ]
    return kernel, scratch


def body(prefill_hidden, decode_hidden, lm_head, prefill_targets, decode_targets, decode_live):
    nx, nz = lax.axis_size("dp"), lax.axis_size("z")
    ny, nc = lax.axis_size("y"), lax.axis_size("c")
    pre, dec = prefill_hidden.shape[0], decode_hidden.shape[0]
    rows = pre + dec
    width, vocab = lm_head.shape
    kernel, scratch = make_kernel(nx, nz, ny, nc, rows, dec, width // nc, vocab)
    hbm = pl.BlockSpec(memory_space=pltpu.HBM)
    return pl.pallas_call(
        kernel,
        out_shape=(jax.ShapeDtypeStruct((pre,), jnp.float32),
                   jax.ShapeDtypeStruct((dec,), jnp.float32)),
        in_specs=[hbm] * 6,
        out_specs=(hbm, hbm),
        scratch_shapes=scratch,
        compiler_params=pltpu.CompilerParams(
            collective_id=0, has_side_effects=True, vmem_limit_bytes=60 << 20),
    )(prefill_hidden, decode_hidden, prefill_targets, decode_targets, decode_live, lm_head.T)


def solution(mesh):
    split = Mesh(mesh.devices.reshape(mesh.shape["dp"], 8, 4, 2), DP_VOCAB)
    placed = (
        P(DP_VOCAB, None),
        P(DP_VOCAB, None),
        P("dp", VOCAB),
        P(DP_VOCAB),
        P(DP_VOCAB),
        P("dp"),
    )
    return jax.shard_map(
        body, mesh=split, in_specs=placed, out_specs=(P(DP_VOCAB), P(DP_VOCAB)), check_vma=False
    )
```

```python
import jax
import jax.numpy as jnp
from jax import lax
from jax.experimental import pallas as pl
from jax.experimental.pallas import tpu as pltpu
from jax.sharding import Mesh
from jax.sharding import PartitionSpec as P

VOCAB = ("z", "y", "c")
DP_VOCAB = ("dp", "z", "y", "c")
MESH = pl.DeviceIdType.MESH
LANES = 128
CHUNK = 256
TOP = 32000.0


def make_kernel(nx, nz, ny, nc, rows, n_dec, depth, vocab):
    pieces_n = nx * nc
    small = pieces_n * rows
    block = ny * small
    first_n = vocab // 32 * 16
    counts = (first_n, vocab - first_n)
    width = -(-(max(counts) + 1) // 512) * 512
    plane = nz * ny * nc

    def kernel(pre_hbm, dec_hbm, pt_hbm, dt_hbm, live_hbm, w_hbm, pre_hbm_out, dec_hbm_out,
               pre_ref, dec_ref, pt_ref, dt_ref, live_ref, w, pieces, xrecv, f40, ybuf, hall, dense, part, sbuf, rel, rd,
               stat, tt, st, fin, pre_out, dec_out,
               w_sem, in_sem, xs, xr, ys, yr, yf, yfr, ags, agr, d2s, d2r, ts, tr, rs, rlr, rdr,
               fs, fr):
        x = lax.axis_index("dp")
        z = lax.axis_index("z")
        y = lax.axis_index("y")
        c = lax.axis_index("c")
        other = 1 - c
        me = x * nc + c
        x_up = (lax.rem(x + 1, nx), z, y, c)
        x_down = (lax.rem(x + nx - 1, nx), z, y, c)
        w_copy = pltpu.make_async_copy(w_hbm, w, w_sem)
        w_copy.start()
        inputs = [pltpu.make_async_copy(src, dst, in_sem.at[k]) for k, (src, dst) in enumerate(
            ((pre_hbm, pre_ref), (dec_hbm, dec_ref), (pt_hbm, pt_ref), (dt_hbm, dt_ref),
             (live_hbm, live_ref)))]
        for copy in inputs:
            copy.start()

        def send(src, dst, ssem, rsem, dev):
            return pltpu.make_async_remote_copy(
                src_ref=src, dst_ref=dst, send_sem=ssem, recv_sem=rsem,
                device_id=dev, device_id_type=MESH)

        def arrival(dst, sem):
            return send(dst, dst, sem, sem, (x, z, y, other))

        barrier = pltpu.get_barrier_semaphore()
        peers = []
        for k in range(1, pieces_n):
            p = lax.rem(me + k, pieces_n)
            peers.append((lax.div(p, nc), z, y, lax.rem(p, nc)))
        for k in range(1, ny):
            peers.append((x, z, lax.rem(y + k, ny), c))
        for k in (1, nz - 1):
            peers.append((x, lax.rem(z + k, nz), y, c))
        for dev in peers:
            pl.semaphore_signal(barrier, inc=1, device_id=dev, device_id_type=MESH)

        n_pre = pre_ref.shape[0]
        for copy in inputs:
            copy.wait()
        lane = lax.broadcasted_iota(jnp.int32, (rows, LANES), 1)
        row = lax.broadcasted_iota(jnp.int32, (rows, LANES), 0)
        ids = jnp.zeros((rows, LANES), jnp.int32)
        for r in range(rows):
            ids = jnp.where(row == r, pt_ref[r] if r < n_pre else dt_ref[r - n_pre], ids)
        digits = jnp.where(lane == 0, ids % 256,
                           jnp.where(lane == 1, (ids // 256) % 256,
                                     jnp.where(lane == 2, ids // 65536, 0))).astype(jnp.float32)
        for p in range(pieces_n):
            cols = slice(p * depth, (p + 1) * depth)
            own = jnp.concatenate([pre_ref[:, cols].astype(jnp.float32),
                                   dec_ref[:, cols].astype(jnp.float32)], axis=0)
            pieces[p, :, 0:depth] = own.astype(jnp.bfloat16)
            pieces[p, :, depth:depth + LANES] = digits.astype(jnp.bfloat16)
        for k in range(nz):
            for h in range(2):
                part[k, h, :, width - LANES:width] = jnp.zeros((block, LANES), jnp.float32)
        stat[...] = jnp.zeros(stat.shape, jnp.float32)

        pl.semaphore_wait(barrier, len(peers))

        def x_copy(k):
            p = lax.rem(me + k, pieces_n)
            return send(pieces.at[p], xrecv.at[me], xs, xr,
                        (lax.div(p, nc), z, y, lax.rem(p, nc)))

        for k in range(1, pieces_n):
            x_copy(k).start()
        xrecv[me] = pieces[me]
        arrival(xrecv.at[0:pieces_n - 1], xr).wait_recv()
        for s in range(pieces_n):
            f40[s * rows:(s + 1) * rows, :] = xrecv[s].astype(jnp.float32)

        ybuf[y] = f40[...].astype(jnp.bfloat16)
        up, down = lax.rem(y + 1, ny), lax.rem(y + ny - 1, ny)
        mid = (depth + LANES) // 2

        def y_part(slot, k):
            return ybuf.at[slot, :, pl.ds(k * mid, mid)]

        def y_copy(way, k):
            return send(y_part(y, k), y_part(y, k), ys, yr.at[way, k],
                        (x, z, up if way else down, c))

        def y_forward(way):
            src = y_part(down if way else up, way)
            return send(src, src, yf, yfr.at[way], (x, z, up if way else down, c))

        above_z, below_z = lax.rem(z + 1, nz), lax.rem(z + nz - 1, nz)

        def spread(j):
            src = ybuf.at[j, :, pl.ds(0, depth)]
            for zz in (above_z, below_z):
                send(src, hall.at[c, z, j], ags, agr.at[z, j], (x, zz, y, c)).start()
            send(src, hall.at[c, z, j], d2s, d2r.at[z], (x, z, y, other)).start()
            hall[c, z, j] = ybuf[j, :, 0:depth]

        def take(dist, parts):
            up_zb, down_zb = lax.rem(z + dist, nz), lax.rem(z + nz - dist, nz)

            def ring(zb, j, zz):
                return send(hall.at[c, zb, j], hall.at[c, zb, j], ags, agr.at[zb, j],
                            (x, zz, y, c))

            def got_rows(zb, j):
                arrival(hall.at[c, zb, j], agr.at[zb, j]).wait_recv()

            def core_copy(zb, j):
                return send(hall.at[c, zb, j], hall.at[c, zb, j], d2s, d2r.at[zb],
                            (x, z, y, other))

            for j in parts:
                got_rows(up_zb, j)

                @pl.when(dist < nz // 2)
                def _():
                    ring(up_zb, j, below_z).start()
                    got_rows(down_zb, j)

                @pl.when(dist < nz // 2 - 1)
                def _():
                    ring(down_zb, j, above_z).start()

                core_copy(up_zb, j).start()

                @pl.when(dist < nz // 2)
                def _():
                    core_copy(down_zb, j).start()

        for far_half in (True, False):
            for way in (1, 0):
                y_copy(way, way if far_half else 1 - way).start()
        spread(y)
        for way in (1, 0):
            arrival(y_part(down if way else up, way), yr.at[way, way]).wait_recv()
            y_forward(way).start()
        for way in (1, 0):
            arrival(y_part(down if way else up, 1 - way), yr.at[way, 1 - way]).wait_recv()
            spread(down if way else up)
        far = lax.rem(y + 2, ny)
        for way in (1, 0):
            arrival(y_part(far, way), yfr.at[way]).wait_recv()
        spread(far)
        one_hop = z * 0 + 1
        take(one_hop, (y,))

        digit = lax.broadcasted_iota(jnp.int32, (small, LANES), 1)
        weight = jnp.where(digit == 0, 1.0, jnp.where(digit == 1, 256.0,
                                                      jnp.where(digit == 2, 65536.0, 0.0)))
        mine_digits = ybuf[x, :, depth:depth + LANES].astype(jnp.float32)
        named = jnp.sum(mine_digits * weight, axis=1, keepdims=True)
        stat[0:small, :] = jnp.broadcast_to(named, (small, LANES))
        tt[z] = jnp.transpose(stat[...])[0:8, :]

        def t_copy(k):
            zz = lax.rem(z + k, nz)
            return send(tt.at[z], tt.at[z], ts, tr, (x, zz, y, c))

        w_copy.wait()

        def block_of(i):
            odd = lax.rem(i, 2)
            dist = lax.div(i + 1, 2)
            return lax.rem(z + nz + jnp.where(odd == 1, dist, -dist), nz)

        def product(rows_of, columns_of):
            return lax.dot_general(rows_of, columns_of, (((1,), (1,)), ((), ())),
                                   preferred_element_type=jnp.float32)

        def align(blocks):
            for k in range(2):
                for c0 in range(0, depth, LANES):
                    rows_of = jnp.concatenate([hall[k, zb, j, :, c0:c0 + LANES].astype(jnp.float32)
                                               for zb in blocks for j in range(ny)], axis=0)
                    dense[k, 0:len(blocks) * block, c0:c0 + LANES] = rows_of.astype(jnp.bfloat16)

        def multiply(blocks, h):
            base = h * first_n
            n_rows = len(blocks) * block
            for n0 in range(0, counts[h], 512):
                n1 = min(n0 + 512, counts[h])
                at = slice(base + n0, base + n1)
                acc = (product(dense[0, 0:n_rows], w[at, 0:depth])
                       + product(dense[1, 0:n_rows], w[at, depth:2 * depth]))
                for j, zb in enumerate(blocks):
                    part[zb, h, :, n0:n1] = acc[j * block:(j + 1) * block]

        def rows_at(q):
            return pl.ds(pl.multiple_of(q * small, 8), small)

        def step_of(code, h):
            return jnp.exp2(code[:, LANES - 1:LANES].astype(jnp.int32).astype(jnp.float32))

        def unpack(code, n0, h, step):
            v = code.astype(jnp.int32).astype(jnp.float32) * step
            if n0 + CHUNK > counts[h]:
                col = lax.broadcasted_iota(jnp.int32, v.shape, 1)
                v = jnp.where(col >= counts[h] - n0, 0.0, v)
            return v

        def quantise(zb, h, q, slot, relayed):
            at = rows_at(q)
            big = jnp.zeros((small, LANES), jnp.float32)
            if relayed:
                step = step_of(rel[zb, h, :, width - LANES:width], h)
            for n0 in range(0, width, CHUNK):
                v = part[zb, h, at, n0:n0 + CHUNK]
                if relayed:
                    v = v + unpack(rel[zb, h, :, n0:n0 + CHUNK], n0, h, step)
                    part[zb, h, at, n0:n0 + CHUNK] = v
                for k in range(0, CHUNK, LANES):
                    big = jnp.maximum(big, jnp.abs(v[:, k:k + LANES]))
            big = jnp.max(big, axis=1, keepdims=True)
            e = jnp.ceil(jnp.log2(jnp.maximum(big, 1e-20) * (1.0 / TOP)))
            scale = jnp.exp2(-e)
            for n0 in range(0, width, CHUNK):
                v = jnp.round(part[zb, h, at, n0:n0 + CHUNK] * scale)
                if n0 + CHUNK > counts[h]:
                    col = lax.broadcasted_iota(jnp.int32, v.shape, 1)
                    v = jnp.where(col >= counts[h] - n0, e, v)
                sbuf[zb, slot, :, n0:n0 + CHUNK] = v.astype(jnp.int32).astype(jnp.int16)

        toward_left = lax.rem(x + nx - 1, nx)
        toward_right = lax.rem(x + 1, nx)
        opposite = lax.rem(x + 2, nx)

        def message(zb, slot):
            if slot == 0:
                dst, rsem, dev = rel.at[zb, 0], rlr.at[zb, 0], x_down
            elif slot == 1:
                dst, rsem, dev = rel.at[zb, 1], rlr.at[zb, 1], x_up
            elif slot in (2, 4):
                h = 1 if slot == 2 else 0
                dst, rsem, dev = rd.at[zb, 0, h], rdr.at[zb], x_down
            else:
                h = 0 if slot == 3 else 1
                dst, rsem, dev = rd.at[zb, 1, h], rdr.at[zb], x_up
            return send(sbuf.at[zb, slot], dst, rs, rsem, dev)

        def emit(zb, h, slots):
            for slot in slots:
                quantise(zb, h, {2: toward_left, 3: toward_right}.get(slot, opposite), slot, False)
                message(zb, slot).start()

        def pass_on(zb):
            arrival(rel.at[zb, 0], rlr.at[zb, 0]).wait_recv()
            quantise(zb, 0, toward_left, 4, True)
            message(zb, 4).start()
            arrival(rel.at[zb, 1], rlr.at[zb, 1]).wait_recv()
            quantise(zb, 1, toward_right, 5, True)
            message(zb, 5).start()

        def pass_pair(dist):
            def one(j, carry):
                pass_on(lax.rem(z + nz + jnp.where(j == 0, dist, -dist), nz))
                return carry

            lax.fori_loop(0, 2, one, 0)

        arrival(hall.at[other, z], d2r.at[z]).wait_recv()
        for h in range(2):
            if h == 0:
                align([z])
            multiply([z], h)
            emit(z, h, (h, 3 - h))
            take(one_hop, (up, down) if h == 0 else (far,))

        def pair(dist, carry):
            above = lax.rem(z + dist, nz)
            below = lax.rem(z + nz - dist, nz)
            t_copy(dist).start()
            t_copy(nz - dist).start()

            arrival(hall.at[other, above], d2r.at[above]).wait_recv()
            arrival(hall.at[other, below], d2r.at[below]).wait_recv()
            for h in range(2):
                if h == 0:
                    align([above, below])
                multiply([above, below], h)

                def one(j, carry):
                    zb = jnp.where(j == 0, above, below)
                    emit(zb, h, (h,))

                    @pl.when(dist > 1)
                    def _():
                        emit(zb, h, (3 - h,))

                    return carry

                lax.fori_loop(0, 2, one, 0)
                take(dist + 1, (y, up) if h == 0 else (down, far))
                if h == 0:
                    @pl.when(dist == 1)
                    def _():
                        pass_on(z)

                    @pl.when(dist > 1)
                    def _():
                        pass_pair(dist - 1)

            return carry

        lax.fori_loop(1, nz // 2, pair, 0)
        across = lax.rem(z + nz // 2, nz)
        t_copy(nz // 2).start()
        arrival(hall.at[other, across], d2r.at[across]).wait_recv()
        for h in range(2):
            if h == 0:
                align([across])
            multiply([across], h)
            emit(across, h, (h,))
        pass_pair(nz // 2 - 1)
        for h in range(2):
            emit(across, h, (3 - h,))

        first = (((z * ny + y) * nc + c) * vocab).astype(jnp.float32)
        mine = (z * ny + y) * nc + c
        at_row = rows_at(x)

        def f_copy(zb, p):
            return send(st.at[zb], fin.at[mine], fs, fr, (lax.div(p, nc), zb, x, lax.rem(p, nc)))

        def reduce(i, carry):
            zb = block_of(i)
            arrival(rd.at[zb], rdr.at[zb]).wait_recv()
            wanted = jnp.transpose(jnp.broadcast_to(tt[zb, 0:1, :], (LANES, LANES)))[0:small, 0:1]
            big = jnp.full((small, LANES), -jnp.inf, jnp.float32)
            picked = jnp.zeros((small, LANES), jnp.float32)
            for h in range(2):
                steps = [step_of(rd[zb, side, h, :, width - LANES:width], h) for side in range(2)]
                local = (wanted - (first + float(h * first_n))).astype(jnp.int32)
                local = jnp.where(jnp.logical_and(local >= 0, local < counts[h]), local, -1)
                for n0 in range(0, width, CHUNK):
                    at = slice(n0, n0 + CHUNK)
                    v = part[zb, h, at_row, at] + (unpack(rd[zb, 0, h, :, at], n0, h, steps[0])
                                                   + unpack(rd[zb, 1, h, :, at], n0, h, steps[1]))
                    col = lax.broadcasted_iota(jnp.int32, v.shape, 1)
                    hit = jnp.where(col == local - n0, v, 0.0)
                    if n0 + CHUNK > counts[h]:
                        v = jnp.where(col >= counts[h] - n0, -jnp.inf, v)
                    part[zb, h, at_row, at] = v
                    for k in range(0, CHUNK, LANES):
                        big = jnp.maximum(big, v[:, k:k + LANES])
                        picked = picked + hit[:, k:k + LANES]
            top = jnp.max(big, axis=1, keepdims=True)
            total = jnp.zeros((small, LANES), jnp.float32)
            for h in range(2):
                for n0 in range(0, width, CHUNK):
                    v = jnp.exp(part[zb, h, at_row, n0:n0 + CHUNK] - top)
                    for k in range(0, CHUNK, LANES):
                        total = total + v[:, k:k + LANES]
            total = jnp.sum(total, axis=1, keepdims=True)
            picked = jnp.sum(picked, axis=1, keepdims=True)
            ln = lax.broadcasted_iota(jnp.int32, (small, LANES), 1)
            stat[0:small, :] = jnp.where(ln == 0, top, jnp.where(ln == 1, total,
                                                                jnp.where(ln == 2, picked, 0.0)))
            tile = jnp.transpose(stat[...])[0:8, :]
            ln = lax.broadcasted_iota(jnp.int32, (1, LANES), 1)
            tile = jnp.where(ln < small, tile[0:1, :],
                             jnp.where(ln < 2 * small, pltpu.roll(tile, small, 1)[1:2, :],
                                       pltpu.roll(tile, 2 * small, 1)[2:3, :]))
            st[zb] = tile
            own_rows = jnp.logical_and(z == zb, y == x)

            @pl.when(own_rows)
            def _():
                fin[mine] = tile

            @pl.when(jnp.logical_not(own_rows))
            def _():
                f_copy(zb, me).start()

            for k in range(1, pieces_n):
                f_copy(zb, lax.rem(me + k, pieces_n)).start()
            return carry

        arrival(tt.at[0:nz - 1], tr).wait_recv()
        reduce(0, 0)
        lax.fori_loop(3, nz - 2, reduce, 0)
        pass_on(across)

        def near(j, carry):
            zb = block_of(j)
            for h in range(2):
                emit(zb, h, (3 - h,))
            return carry

        lax.fori_loop(1, 3, near, 0)
        lax.fori_loop(nz - 2, nz, reduce, 0)
        lax.fori_loop(1, 3, reduce, 0)
        def left(ref, sem):
            send(ref, ref, sem, sem, (x, z, y, other)).wait_send()

        owner = x == y
        left(pieces.at[0:pieces_n - 1], xs)
        left(ybuf.at[0:2], ys)
        left(ybuf.at[0], yf)
        left(hall.at[c, 0:nz - 1], ags)
        left(hall.at[c], d2s)
        left(tt.at[0:nz - 1], ts)
        left(sbuf, rs)

        @pl.when(owner)
        def _():
            left(fin.at[0:plane - 1], fs)
            arrival(fin.at[0:plane - 1], fr).wait_recv()

        @pl.when(jnp.logical_not(owner))
        def _():
            left(fin, fs)
            arrival(fin, fr).wait_recv()

        tops = fin[:, 0, :]
        top = jnp.max(tops, axis=0, keepdims=True)
        weights = jnp.exp(tops - top)
        total = jnp.sum(pltpu.roll(tops, LANES - small, 1) * weights, axis=0, keepdims=True)
        picked = jnp.sum(pltpu.roll(tops, LANES - 2 * small, 1), axis=0, keepdims=True)
        joined = jnp.broadcast_to(picked - (top + jnp.log(total)), (8, LANES))
        values = pltpu.roll(joined, LANES - me * rows, 1)
        lanes = lax.broadcasted_iota(jnp.int32, (8, LANES), 1)
        position = mine * n_dec + lanes - n_pre
        values = jnp.where(jnp.logical_and(lanes >= n_pre, position >= live_ref[0]), 0.0, values)
        pre_out[...] = values[0, 0:n_pre]
        dec_out[...] = values[0, n_pre:rows]
        outputs = [pltpu.make_async_copy(pre_out, pre_hbm_out, in_sem.at[0]),
                   pltpu.make_async_copy(dec_out, dec_hbm_out, in_sem.at[1])]
        for copy in outputs:
            copy.start()

        for copy in outputs:
            copy.wait()

    f32, bf16, i16 = jnp.float32, jnp.bfloat16, jnp.int16
    dma = pltpu.SemaphoreType.DMA
    scratch = [
        pltpu.VMEM((rows - n_dec, nx * nc * depth), bf16),
        pltpu.VMEM((n_dec, nx * nc * depth), bf16),
        pltpu.SMEM((rows - n_dec,), jnp.int32),
        pltpu.SMEM((n_dec,), jnp.int32),
        pltpu.SMEM((1,), jnp.int32),
        pltpu.VMEM((vocab, 2 * depth), bf16),
        pltpu.VMEM((pieces_n, rows, depth + LANES), bf16),
        pltpu.VMEM((pieces_n, rows, depth + LANES), bf16),
        pltpu.VMEM((small, depth + LANES), f32),
        pltpu.VMEM((ny, small, depth + LANES), bf16),
        pltpu.VMEM((nc, nz, ny, small, depth), bf16),
        pltpu.VMEM((2, 2 * block, depth), bf16),
        pltpu.VMEM((nz, 2, block, width), f32),
        pltpu.VMEM((nz, 6, small, width), i16),
        pltpu.VMEM((nz, 2, small, width), i16),
        pltpu.VMEM((nz, 2, 2, small, width), i16),
        pltpu.VMEM((LANES, LANES), f32),
        pltpu.VMEM((nz, 8, LANES), f32),
        pltpu.VMEM((nz, 1, LANES), f32),
        pltpu.VMEM((plane, 1, LANES), f32),
        pltpu.VMEM((rows - n_dec,), f32),
        pltpu.VMEM((n_dec,), f32),
        dma, dma((5,)), dma, dma, dma, dma((2, 2)), dma, dma((2,)),
        dma, dma((nz, ny)), dma, dma((nz,)), dma, dma,
        dma, dma((nz, 2)), dma((nz,)),
        dma, dma,
    ]
    return kernel, scratch


def body(prefill_hidden, decode_hidden, lm_head, prefill_targets, decode_targets, decode_live):
    nx, nz = lax.axis_size("dp"), lax.axis_size("z")
    ny, nc = lax.axis_size("y"), lax.axis_size("c")
    pre, dec = prefill_hidden.shape[0], decode_hidden.shape[0]
    rows = pre + dec
    width, vocab = lm_head.shape
    kernel, scratch = make_kernel(nx, nz, ny, nc, rows, dec, width // nc, vocab)
    hbm = pl.BlockSpec(memory_space=pltpu.HBM)
    return pl.pallas_call(
        kernel,
        out_shape=(jax.ShapeDtypeStruct((pre,), jnp.float32),
                   jax.ShapeDtypeStruct((dec,), jnp.float32)),
        in_specs=[hbm] * 6,
        out_specs=(hbm, hbm),
        scratch_shapes=scratch,
        compiler_params=pltpu.CompilerParams(
            collective_id=0, has_side_effects=True, vmem_limit_bytes=60 << 20),
    )(prefill_hidden, decode_hidden, prefill_targets, decode_targets, decode_live, lm_head.T)


def solution(mesh):
    split = Mesh(mesh.devices.reshape(mesh.shape["dp"], 8, 4, 2), DP_VOCAB)
    placed = (
        P(DP_VOCAB, None),
        P(DP_VOCAB, None),
        P("dp", VOCAB),
        P(DP_VOCAB),
        P(DP_VOCAB),
        P("dp"),
    )
    return jax.shard_map(
        body, mesh=split, in_specs=placed, out_specs=(P(DP_VOCAB), P(DP_VOCAB)), check_vma=False
    )
```

```python
import jax
import jax.numpy as jnp
from jax import lax
from jax.experimental import pallas as pl
from jax.experimental.pallas import tpu as pltpu
from jax.sharding import Mesh
from jax.sharding import PartitionSpec as P

VOCAB = ("z", "y", "c")
DP_VOCAB = ("dp", "z", "y", "c")
MESH = pl.DeviceIdType.MESH
LANES = 128
CHUNK = 256
TOP = 32000.0


def make_kernel(nx, nz, ny, nc, rows, n_dec, depth, vocab):
    pieces_n = nx * nc
    small = pieces_n * rows
    block = ny * small
    first_n = vocab // 32 * 16
    counts = (first_n, vocab - first_n)
    width = -(-(max(counts) + 1) // 512) * 512
    plane = nz * ny * nc

    def kernel(pre_hbm, dec_hbm, pt_hbm, dt_hbm, live_hbm, w_hbm, pre_hbm_out, dec_hbm_out,
               pre_ref, dec_ref, pt_ref, dt_ref, live_ref, w, pieces, xrecv, f40, ybuf, hall, dense, part, sbuf, rel, rd,
               stat, tt, st, fin, pre_out, dec_out,
               w_sem, in_sem, xs, xr, ys, yr, yf, yfr, ags, agr, d2s, d2r, ts, tr, rs, rlr, rdr,
               fs, fr):
        x = lax.axis_index("dp")
        z = lax.axis_index("z")
        y = lax.axis_index("y")
        c = lax.axis_index("c")
        other = 1 - c
        me = x * nc + c
        x_up = (lax.rem(x + 1, nx), z, y, c)
        x_down = (lax.rem(x + nx - 1, nx), z, y, c)
        w_copy = pltpu.make_async_copy(w_hbm, w, w_sem)
        w_copy.start()
        inputs = [pltpu.make_async_copy(src, dst, in_sem.at[k]) for k, (src, dst) in enumerate(
            ((pre_hbm, pre_ref), (dec_hbm, dec_ref), (pt_hbm, pt_ref), (dt_hbm, dt_ref),
             (live_hbm, live_ref)))]
        for copy in inputs:
            copy.start()

        def send(src, dst, ssem, rsem, dev):
            return pltpu.make_async_remote_copy(
                src_ref=src, dst_ref=dst, send_sem=ssem, recv_sem=rsem,
                device_id=dev, device_id_type=MESH)

        def arrival(dst, sem):
            return send(dst, dst, sem, sem, (x, z, y, other))

        barrier = pltpu.get_barrier_semaphore()
        peers = []
        for k in range(1, pieces_n):
            p = lax.rem(me + k, pieces_n)
            peers.append((lax.div(p, nc), z, y, lax.rem(p, nc)))
        for k in range(1, ny):
            peers.append((x, z, lax.rem(y + k, ny), c))
        for k in (1, nz - 1):
            peers.append((x, lax.rem(z + k, nz), y, c))
        for dev in peers:
            pl.semaphore_signal(barrier, inc=1, device_id=dev, device_id_type=MESH)

        n_pre = pre_ref.shape[0]
        for copy in inputs:
            copy.wait()
        lane = lax.broadcasted_iota(jnp.int32, (rows, LANES), 1)
        row = lax.broadcasted_iota(jnp.int32, (rows, LANES), 0)
        ids = jnp.zeros((rows, LANES), jnp.int32)
        for r in range(rows):
            ids = jnp.where(row == r, pt_ref[r] if r < n_pre else dt_ref[r - n_pre], ids)
        digits = jnp.where(lane == 0, ids % 256,
                           jnp.where(lane == 1, (ids // 256) % 256,
                                     jnp.where(lane == 2, ids // 65536, 0))).astype(jnp.float32)
        for p in range(pieces_n):
            cols = slice(p * depth, (p + 1) * depth)
            own = jnp.concatenate([pre_ref[:, cols].astype(jnp.float32),
                                   dec_ref[:, cols].astype(jnp.float32)], axis=0)
            pieces[p, :, 0:depth] = own.astype(jnp.bfloat16)
            pieces[p, :, depth:depth + LANES] = digits.astype(jnp.bfloat16)
        for k in range(nz):
            for h in range(2):
                part[k, h, :, width - LANES:width] = jnp.zeros((block, LANES), jnp.float32)
        stat[...] = jnp.zeros(stat.shape, jnp.float32)

        pl.semaphore_wait(barrier, len(peers))

        def x_copy(k):
            p = lax.rem(me + k, pieces_n)
            return send(pieces.at[p], xrecv.at[me], xs, xr,
                        (lax.div(p, nc), z, y, lax.rem(p, nc)))

        for k in range(1, pieces_n):
            x_copy(k).start()
        xrecv[me] = pieces[me]
        arrival(xrecv.at[0:pieces_n - 1], xr).wait_recv()
        for s in range(pieces_n):
            f40[s * rows:(s + 1) * rows, :] = xrecv[s].astype(jnp.float32)

        ybuf[y] = f40[...].astype(jnp.bfloat16)
        up, down = lax.rem(y + 1, ny), lax.rem(y + ny - 1, ny)
        mid = (depth + LANES) // 2

        def y_part(slot, k):
            return ybuf.at[slot, :, pl.ds(k * mid, mid)]

        def y_copy(way, k):
            return send(y_part(y, k), y_part(y, k), ys, yr.at[way, k],
                        (x, z, up if way else down, c))

        def y_forward(way):
            src = y_part(down if way else up, way)
            return send(src, src, yf, yfr.at[way], (x, z, up if way else down, c))

        above_z, below_z = lax.rem(z + 1, nz), lax.rem(z + nz - 1, nz)

        def spread(j):
            src = ybuf.at[j, :, pl.ds(0, depth)]
            for zz in (above_z, below_z):
                send(src, hall.at[c, z, j], ags, agr.at[z, j], (x, zz, y, c)).start()
            send(src, hall.at[c, z, j], d2s, d2r.at[z], (x, z, y, other)).start()
            hall[c, z, j] = ybuf[j, :, 0:depth]

        def take(dist, parts):
            up_zb, down_zb = lax.rem(z + dist, nz), lax.rem(z + nz - dist, nz)

            def ring(zb, j, zz):
                return send(hall.at[c, zb, j], hall.at[c, zb, j], ags, agr.at[zb, j],
                            (x, zz, y, c))

            def got_rows(zb, j):
                arrival(hall.at[c, zb, j], agr.at[zb, j]).wait_recv()

            def core_copy(zb, j):
                return send(hall.at[c, zb, j], hall.at[c, zb, j], d2s, d2r.at[zb],
                            (x, z, y, other))

            for j in parts:
                got_rows(up_zb, j)

                @pl.when(dist < nz // 2)
                def _():
                    ring(up_zb, j, below_z).start()
                    got_rows(down_zb, j)

                @pl.when(dist < nz // 2 - 1)
                def _():
                    ring(down_zb, j, above_z).start()

                core_copy(up_zb, j).start()

                @pl.when(dist < nz // 2)
                def _():
                    core_copy(down_zb, j).start()

        for far_half in (True, False):
            for way in (1, 0):
                y_copy(way, way if far_half else 1 - way).start()
        spread(y)
        for way in (1, 0):
            arrival(y_part(down if way else up, way), yr.at[way, way]).wait_recv()
            y_forward(way).start()
        for way in (1, 0):
            arrival(y_part(down if way else up, 1 - way), yr.at[way, 1 - way]).wait_recv()
            spread(down if way else up)
        far = lax.rem(y + 2, ny)
        for way in (1, 0):
            arrival(y_part(far, way), yfr.at[way]).wait_recv()
        spread(far)
        one_hop = z * 0 + 1
        take(one_hop, (y,))

        digit = lax.broadcasted_iota(jnp.int32, (small, LANES), 1)
        weight = jnp.where(digit == 0, 1.0, jnp.where(digit == 1, 256.0,
                                                      jnp.where(digit == 2, 65536.0, 0.0)))
        mine_digits = ybuf[x, :, depth:depth + LANES].astype(jnp.float32)
        named = jnp.sum(mine_digits * weight, axis=1, keepdims=True)
        stat[0:small, :] = jnp.broadcast_to(named, (small, LANES))
        tt[z] = jnp.transpose(stat[...])[0:8, :]

        def t_copy(k):
            zz = lax.rem(z + k, nz)
            return send(tt.at[z], tt.at[z], ts, tr, (x, zz, y, c))

        w_copy.wait()

        def block_of(i):
            odd = lax.rem(i, 2)
            dist = lax.div(i + 1, 2)
            return lax.rem(z + nz + jnp.where(odd == 1, dist, -dist), nz)

        def product(rows_of, columns_of):
            return lax.dot_general(rows_of, columns_of, (((1,), (1,)), ((), ())),
                                   preferred_element_type=jnp.float32)

        def align(blocks):
            for k in range(2):
                for c0 in range(0, depth, LANES):
                    rows_of = jnp.concatenate([hall[k, zb, j, :, c0:c0 + LANES].astype(jnp.float32)
                                               for zb in blocks for j in range(ny)], axis=0)
                    dense[k, 0:len(blocks) * block, c0:c0 + LANES] = rows_of.astype(jnp.bfloat16)

        def multiply(blocks, h):
            base = h * first_n
            n_rows = len(blocks) * block
            for n0 in range(0, counts[h], 512):
                n1 = min(n0 + 512, counts[h])
                at = slice(base + n0, base + n1)
                acc = (product(dense[0, 0:n_rows], w[at, 0:depth])
                       + product(dense[1, 0:n_rows], w[at, depth:2 * depth]))
                for j, zb in enumerate(blocks):
                    part[zb, h, :, n0:n1] = acc[j * block:(j + 1) * block]

        def rows_at(q):
            return pl.ds(pl.multiple_of(q * small, 8), small)

        def step_of(code, h):
            return jnp.exp2(code[:, LANES - 1:LANES].astype(jnp.int32).astype(jnp.float32))

        def unpack(code, n0, h, step):
            v = code.astype(jnp.int32).astype(jnp.float32) * step
            if n0 + CHUNK > counts[h]:
                col = lax.broadcasted_iota(jnp.int32, v.shape, 1)
                v = jnp.where(col >= counts[h] - n0, 0.0, v)
            return v

        def quantise(zb, h, q, slot, relayed):
            at = rows_at(q)
            big = jnp.zeros((small, LANES), jnp.float32)
            if relayed:
                step = step_of(rel[zb, h, :, width - LANES:width], h)
            for n0 in range(0, width, CHUNK):
                v = part[zb, h, at, n0:n0 + CHUNK]
                if relayed:
                    v = v + unpack(rel[zb, h, :, n0:n0 + CHUNK], n0, h, step)
                    part[zb, h, at, n0:n0 + CHUNK] = v
                for k in range(0, CHUNK, LANES):
                    big = jnp.maximum(big, jnp.abs(v[:, k:k + LANES]))
            big = jnp.max(big, axis=1, keepdims=True)
            e = jnp.ceil(jnp.log2(jnp.maximum(big, 1e-20) * (1.0 / TOP)))
            scale = jnp.exp2(-e)
            for n0 in range(0, width, CHUNK):
                v = jnp.round(part[zb, h, at, n0:n0 + CHUNK] * scale)
                if n0 + CHUNK > counts[h]:
                    col = lax.broadcasted_iota(jnp.int32, v.shape, 1)
                    v = jnp.where(col >= counts[h] - n0, e, v)
                sbuf[zb, slot, :, n0:n0 + CHUNK] = v.astype(jnp.int32).astype(jnp.int16)

        toward_left = lax.rem(x + nx - 1, nx)
        toward_right = lax.rem(x + 1, nx)
        opposite = lax.rem(x + 2, nx)

        def message(zb, slot):
            if slot == 0:
                dst, rsem, dev = rel.at[zb, 0], rlr.at[zb, 0], x_down
            elif slot == 1:
                dst, rsem, dev = rel.at[zb, 1], rlr.at[zb, 1], x_up
            elif slot in (2, 4):
                h = 1 if slot == 2 else 0
                dst, rsem, dev = rd.at[zb, 0, h], rdr.at[zb], x_down
            else:
                h = 0 if slot == 3 else 1
                dst, rsem, dev = rd.at[zb, 1, h], rdr.at[zb], x_up
            return send(sbuf.at[zb, slot], dst, rs, rsem, dev)

        def emit(zb, h, slots):
            for slot in slots:
                quantise(zb, h, {2: toward_left, 3: toward_right}.get(slot, opposite), slot, False)
                message(zb, slot).start()

        def pass_on(zb):
            arrival(rel.at[zb, 0], rlr.at[zb, 0]).wait_recv()
            quantise(zb, 0, toward_left, 4, True)
            message(zb, 4).start()
            arrival(rel.at[zb, 1], rlr.at[zb, 1]).wait_recv()
            quantise(zb, 1, toward_right, 5, True)
            message(zb, 5).start()

        def pass_pair(dist):
            def one(j, carry):
                pass_on(lax.rem(z + nz + jnp.where(j == 0, dist, -dist), nz))
                return carry

            lax.fori_loop(0, 2, one, 0)

        arrival(hall.at[other, z], d2r.at[z]).wait_recv()
        for h in range(2):
            if h == 0:
                align([z])
            multiply([z], h)
            emit(z, h, (h, 3 - h))
            take(one_hop, (up, down) if h == 0 else (far,))

        def pair(dist, carry):
            above = lax.rem(z + dist, nz)
            below = lax.rem(z + nz - dist, nz)
            t_copy(dist).start()
            t_copy(nz - dist).start()

            arrival(hall.at[other, above], d2r.at[above]).wait_recv()
            arrival(hall.at[other, below], d2r.at[below]).wait_recv()
            for h in range(2):
                if h == 0:
                    align([above, below])
                multiply([above, below], h)

                def one(j, carry):
                    zb = jnp.where(j == 0, above, below)
                    emit(zb, h, (h,))

                    @pl.when(dist > j)
                    def _():
                        emit(zb, h, (3 - h,))

                    return carry

                lax.fori_loop(0, 2, one, 0)
                take(dist + 1, (y, up) if h == 0 else (down, far))
                if h == 0:
                    @pl.when(dist == 1)
                    def _():
                        pass_on(z)

                    @pl.when(dist > 1)
                    def _():
                        pass_pair(dist - 1)

            return carry

        lax.fori_loop(1, nz // 2, pair, 0)
        across = lax.rem(z + nz // 2, nz)
        t_copy(nz // 2).start()
        arrival(hall.at[other, across], d2r.at[across]).wait_recv()
        for h in range(2):
            if h == 0:
                align([across])
            multiply([across], h)
            emit(across, h, (h,))
        pass_pair(nz // 2 - 1)
        for h in range(2):
            emit(across, h, (3 - h,))

        first = (((z * ny + y) * nc + c) * vocab).astype(jnp.float32)
        mine = (z * ny + y) * nc + c
        at_row = rows_at(x)

        def f_copy(zb, p):
            return send(st.at[zb], fin.at[mine], fs, fr, (lax.div(p, nc), zb, x, lax.rem(p, nc)))

        def reduce(i, carry):
            zb = block_of(i)
            arrival(rd.at[zb], rdr.at[zb]).wait_recv()
            wanted = jnp.transpose(jnp.broadcast_to(tt[zb, 0:1, :], (LANES, LANES)))[0:small, 0:1]
            big = jnp.full((small, LANES), -jnp.inf, jnp.float32)
            picked = jnp.zeros((small, LANES), jnp.float32)
            for h in range(2):
                steps = [step_of(rd[zb, side, h, :, width - LANES:width], h) for side in range(2)]
                local = (wanted - (first + float(h * first_n))).astype(jnp.int32)
                local = jnp.where(jnp.logical_and(local >= 0, local < counts[h]), local, -1)
                for n0 in range(0, width, CHUNK):
                    at = slice(n0, n0 + CHUNK)
                    v = part[zb, h, at_row, at] + (unpack(rd[zb, 0, h, :, at], n0, h, steps[0])
                                                   + unpack(rd[zb, 1, h, :, at], n0, h, steps[1]))
                    col = lax.broadcasted_iota(jnp.int32, v.shape, 1)
                    hit = jnp.where(col == local - n0, v, 0.0)
                    if n0 + CHUNK > counts[h]:
                        v = jnp.where(col >= counts[h] - n0, -jnp.inf, v)
                    part[zb, h, at_row, at] = v
                    for k in range(0, CHUNK, LANES):
                        big = jnp.maximum(big, v[:, k:k + LANES])
                        picked = picked + hit[:, k:k + LANES]
            top = jnp.max(big, axis=1, keepdims=True)
            total = jnp.zeros((small, LANES), jnp.float32)
            for h in range(2):
                for n0 in range(0, width, CHUNK):
                    v = jnp.exp(part[zb, h, at_row, n0:n0 + CHUNK] - top)
                    for k in range(0, CHUNK, LANES):
                        total = total + v[:, k:k + LANES]
            total = jnp.sum(total, axis=1, keepdims=True)
            picked = jnp.sum(picked, axis=1, keepdims=True)
            ln = lax.broadcasted_iota(jnp.int32, (small, LANES), 1)
            stat[0:small, :] = jnp.where(ln == 0, top, jnp.where(ln == 1, total,
                                                                jnp.where(ln == 2, picked, 0.0)))
            tile = jnp.transpose(stat[...])[0:8, :]
            ln = lax.broadcasted_iota(jnp.int32, (1, LANES), 1)
            tile = jnp.where(ln < small, tile[0:1, :],
                             jnp.where(ln < 2 * small, pltpu.roll(tile, small, 1)[1:2, :],
                                       pltpu.roll(tile, 2 * small, 1)[2:3, :]))
            st[zb] = tile
            own_rows = jnp.logical_and(z == zb, y == x)

            @pl.when(own_rows)
            def _():
                fin[mine] = tile

            @pl.when(jnp.logical_not(own_rows))
            def _():
                f_copy(zb, me).start()

            for k in range(1, pieces_n):
                f_copy(zb, lax.rem(me + k, pieces_n)).start()
            return carry

        arrival(tt.at[0:nz - 1], tr).wait_recv()
        lax.fori_loop(0, 2, reduce, 0)
        lax.fori_loop(3, nz - 2, reduce, 0)
        pass_on(across)

        def near(j, carry):
            zb = block_of(j)
            for h in range(2):
                emit(zb, h, (3 - h,))
            return carry

        near(2, 0)
        lax.fori_loop(nz - 2, nz, reduce, 0)
        reduce(2, 0)
        def left(ref, sem):
            send(ref, ref, sem, sem, (x, z, y, other)).wait_send()

        owner = x == y
        left(pieces.at[0:pieces_n - 1], xs)
        left(ybuf.at[0:2], ys)
        left(ybuf.at[0], yf)
        left(hall.at[c, 0:nz - 1], ags)
        left(hall.at[c], d2s)
        left(tt.at[0:nz - 1], ts)
        left(sbuf, rs)

        @pl.when(owner)
        def _():
            left(fin.at[0:plane - 1], fs)
            arrival(fin.at[0:plane - 1], fr).wait_recv()

        @pl.when(jnp.logical_not(owner))
        def _():
            left(fin, fs)
            arrival(fin, fr).wait_recv()

        tops = fin[:, 0, :]
        top = jnp.max(tops, axis=0, keepdims=True)
        weights = jnp.exp(tops - top)
        total = jnp.sum(pltpu.roll(tops, LANES - small, 1) * weights, axis=0, keepdims=True)
        picked = jnp.sum(pltpu.roll(tops, LANES - 2 * small, 1), axis=0, keepdims=True)
        joined = jnp.broadcast_to(picked - (top + jnp.log(total)), (8, LANES))
        values = pltpu.roll(joined, LANES - me * rows, 1)
        lanes = lax.broadcasted_iota(jnp.int32, (8, LANES), 1)
        position = mine * n_dec + lanes - n_pre
        values = jnp.where(jnp.logical_and(lanes >= n_pre, position >= live_ref[0]), 0.0, values)
        pre_out[...] = values[0, 0:n_pre]
        dec_out[...] = values[0, n_pre:rows]
        outputs = [pltpu.make_async_copy(pre_out, pre_hbm_out, in_sem.at[0]),
                   pltpu.make_async_copy(dec_out, dec_hbm_out, in_sem.at[1])]
        for copy in outputs:
            copy.start()

        for copy in outputs:
            copy.wait()

    f32, bf16, i16 = jnp.float32, jnp.bfloat16, jnp.int16
    dma = pltpu.SemaphoreType.DMA
    scratch = [
        pltpu.VMEM((rows - n_dec, nx * nc * depth), bf16),
        pltpu.VMEM((n_dec, nx * nc * depth), bf16),
        pltpu.SMEM((rows - n_dec,), jnp.int32),
        pltpu.SMEM((n_dec,), jnp.int32),
        pltpu.SMEM((1,), jnp.int32),
        pltpu.VMEM((vocab, 2 * depth), bf16),
        pltpu.VMEM((pieces_n, rows, depth + LANES), bf16),
        pltpu.VMEM((pieces_n, rows, depth + LANES), bf16),
        pltpu.VMEM((small, depth + LANES), f32),
        pltpu.VMEM((ny, small, depth + LANES), bf16),
        pltpu.VMEM((nc, nz, ny, small, depth), bf16),
        pltpu.VMEM((2, 2 * block, depth), bf16),
        pltpu.VMEM((nz, 2, block, width), f32),
        pltpu.VMEM((nz, 6, small, width), i16),
        pltpu.VMEM((nz, 2, small, width), i16),
        pltpu.VMEM((nz, 2, 2, small, width), i16),
        pltpu.VMEM((LANES, LANES), f32),
        pltpu.VMEM((nz, 8, LANES), f32),
        pltpu.VMEM((nz, 1, LANES), f32),
        pltpu.VMEM((plane, 1, LANES), f32),
        pltpu.VMEM((rows - n_dec,), f32),
        pltpu.VMEM((n_dec,), f32),
        dma, dma((5,)), dma, dma, dma, dma((2, 2)), dma, dma((2,)),
        dma, dma((nz, ny)), dma, dma((nz,)), dma, dma,
        dma, dma((nz, 2)), dma((nz,)),
        dma, dma,
    ]
    return kernel, scratch


def body(prefill_hidden, decode_hidden, lm_head, prefill_targets, decode_targets, decode_live):
    nx, nz = lax.axis_size("dp"), lax.axis_size("z")
    ny, nc = lax.axis_size("y"), lax.axis_size("c")
    pre, dec = prefill_hidden.shape[0], decode_hidden.shape[0]
    rows = pre + dec
    width, vocab = lm_head.shape
    kernel, scratch = make_kernel(nx, nz, ny, nc, rows, dec, width // nc, vocab)
    hbm = pl.BlockSpec(memory_space=pltpu.HBM)
    return pl.pallas_call(
        kernel,
        out_shape=(jax.ShapeDtypeStruct((pre,), jnp.float32),
                   jax.ShapeDtypeStruct((dec,), jnp.float32)),
        in_specs=[hbm] * 6,
        out_specs=(hbm, hbm),
        scratch_shapes=scratch,
        compiler_params=pltpu.CompilerParams(
            collective_id=0, has_side_effects=True, vmem_limit_bytes=60 << 20),
    )(prefill_hidden, decode_hidden, prefill_targets, decode_targets, decode_live, lm_head.T)


def solution(mesh):
    split = Mesh(mesh.devices.reshape(mesh.shape["dp"], 8, 4, 2), DP_VOCAB)
    placed = (
        P(DP_VOCAB, None),
        P(DP_VOCAB, None),
        P("dp", VOCAB),
        P(DP_VOCAB),
        P(DP_VOCAB),
        P("dp"),
    )
    return jax.shard_map(
        body, mesh=split, in_specs=placed, out_specs=(P(DP_VOCAB), P(DP_VOCAB)), check_vma=False
    )
```
